32 devices in a mesh: farcp: 4 (over x, core), nearcp: 2 (over y), heads: 4 (over z).
Axes of the slice: x: 2, y: 2, z: 4, core: 2. Of those that a mesh axis runs over, the one named last changes fastest.
Arguments:
- raw_keys: bfloat16 [8, 2048, 8, 128], P(None, ('farcp', 'nearcp'), 'heads'), may hold values from -6 to 6
- raw_values: bfloat16 [8, 2048, 8, 128], P(None, ('farcp', 'nearcp'), 'heads'), may hold values from -6 to 6
- turn_angle: float32 [2048, 64], replicated, may hold values from -3.140625 to 3.140625
- key_gain: float32 [128], replicated, may hold values from 0.25 to 1.75
Outputs:
- cache_keys: bfloat16 [8, 2048, 8, 128], P(('farcp', 'nearcp'), None, 'heads')
- cache_values: bfloat16 [8, 2048, 8, 128], P(('farcp', 'nearcp'), None, 'heads')
- key_scale: float32 [8, 8, 128], P(('farcp', 'nearcp'), 'heads')
The draws below stay inside these ranges and needn't reach their ends.
All inputs are finite; a program needn't handle non-finite values. Where the reference program divides by a largest or mean magnitude, that divisor is 1e-20 or more.
Results may differ from the reference program's by a relative error of at most 0.001.
Values may be sent and summed in bfloat16 or wider, within the bound.
A program may use at most 128 MiB of HBM per device.

```python
import jax
import jax.numpy as jnp
from jax import lax

BATCH = 8
LENGTH = 2048
KV_HEADS = 8
HEAD_SIZE = 128
HALF_HEAD = 64


def block_scale(stream_key, dims, split, smallest, largest):
    gain = 1.0
    for position, blocks in split:
        heights = jax.random.uniform(jax.random.fold_in(jax.random.fold_in(stream_key, 6), position), (blocks,), jnp.float32, smallest / len(split), largest / len(split))
        gain = gain * jnp.repeat(jnp.exp(heights), dims[position] // blocks).reshape((-1,) + (1,) * (len(dims) - 1 - position))
    return gain


def normal_values(stream_key, shape, deviation, most, split=(), dtype=jnp.bfloat16):
    result = deviation * jax.random.normal(stream_key, shape, jnp.float32)
    if split:
        result = result * block_scale(stream_key, shape, split, -0.22, 0.18)
    return jnp.clip(result, -most, most).astype(dtype)


def setup_inputs(seed: int = 0) -> dict:
    streams_of = jax.random.split(jax.random.key(seed), 5)
    raw_keys = normal_values(streams_of[0], (BATCH, LENGTH, KV_HEADS, HEAD_SIZE), 1.0, 6.0, ((1, 8), (2, 4)))
    raw_values = normal_values(streams_of[1], (BATCH, LENGTH, KV_HEADS, HEAD_SIZE), 1.0, 6.0, ((1, 8), (2, 4)))
    turn_angle = jnp.clip(jax.random.uniform(streams_of[2], (LENGTH, HALF_HEAD), jnp.float32, -3.140625, 3.140625), -3.140625, 3.140625)
    key_gain = jnp.clip(1.0 + 0.15 * jax.random.normal(streams_of[3], (HEAD_SIZE,), jnp.float32), 0.25, 1.75)
    return dict(raw_keys=raw_keys, raw_values=raw_values, turn_angle=turn_angle, key_gain=key_gain)


def turn_pairs(vectors, angle):
    half = vectors.shape[-1] // 2
    cosine, sine = (jnp.cos(angle)[None, :, None, :], jnp.sin(angle)[None, :, None, :])
    first, second = (vectors[..., :half], vectors[..., half:])
    return jnp.concatenate([first * cosine - second * sine, second * cosine + first * sine], axis=-1)

def unit_rows(vectors, row_gain):
    return vectors * lax.rsqrt(lax.optimization_barrier(jnp.mean(vectors * vectors, axis=-1, keepdims=True)) + 1e-06) * row_gain

def ready_to_store(plain_keys, angle, key_gain):
    wide_keys = plain_keys.astype(jnp.float32)
    wide_keys = unit_rows(wide_keys, key_gain)
    return turn_pairs(wide_keys, angle)

def reference(raw_keys, raw_values, turn_angle, key_gain):
    turned_keys = ready_to_store(raw_keys, turn_angle, key_gain)
    key_scale = lax.optimization_barrier(jnp.max(jnp.abs(turned_keys), axis=1))
    narrow_keys = (turned_keys / key_scale[:, None]).astype(jnp.bfloat16)
    cache_keys = narrow_keys
    cache_values = raw_values
    return (cache_keys, cache_values, key_scale)
```

```python
import functools

import jax
import jax.numpy as jnp
from jax import lax
from jax.experimental import pallas as pl
from jax.experimental.pallas import tpu as pltpu
from jax.sharding import PartitionSpec as P

MESH = pl.DeviceIdType.MESH
LANES = 128
SUBLANES = 8
BLOCK = 128
ROOT, SIDE, END = 0, 1, 2
SINE = (1.0, -0.1666666716337204, 0.008333330973982811, -0.00019840861205011606,
        2.752528644123231e-06, -2.3889498379503493e-08)
COSINE = (1.0, -0.5, 0.0416666679084301, -0.0013888884568586946, 2.4801040126476437e-05,
          -2.752468617472914e-07, 1.9907717696554528e-09)


def polynomial(coefficients, z):
    total = jnp.full_like(z, coefficients[-1])
    for coefficient in coefficients[-2::-1]:
        total = total * z + coefficient
    return total


def cosine_and_sine(angle):
    y = (1.57079637 - jnp.abs(angle)) - 4.371139e-08
    z = y * y
    sine = polynomial(COSINE, z)
    return y * polynomial(SINE, z), jnp.where(angle < 0, -sine, sine)


def partner(index, offset, size):
    result, bit = 0, 1
    while bit < size:
        digit = (index // bit) % 2
        result = result + ((digit + 1) % 2 if offset & bit else digit) * bit
        bit *= 2
    return result


def role_of(far_index, near_index):
    return jnp.where(far_index < 2, 0, 1) + jnp.where(near_index == 0, 0, 1)


def place_of(device):
    return {"farcp": device[0], "nearcp": device[1]}


def kernel(far, near, heads, offsets, keys, values, angle, gain, out_keys, out_values, out_scale,
           landed, held_keys, turned, cosines, sines, angles, gains, send_sem, recv_sem, local_sem, ready):
    members, rows, _ = landed.shape
    far_index, near_index = lax.axis_index("farcp"), lax.axis_index("nearcp")
    me = far_index * near + near_index
    one_link = [o for o in offsets if o[0] < 2 or o[1] == 0]
    two_links = [o for o in offsets if o not in one_link]
    peers = {
        (f, n): (partner(far_index, f, far), partner(near_index, n, near)) for f, n in offsets
    }
    role, roles = role_of(far_index, near_index), {o: role_of(*peers[o]) for o in offsets}
    roots, sides, ends = 2, 2 * (near - 1) + far - 2, (far - 2) * (near - 1)

    def own(i, source, target):
        return pltpu.make_async_copy(source, target, local_sem.at[i])

    local = [
        own(0, angle, angles),
        own(1, gain, gains),
        own(2, keys.at[me], held_keys.at[me]),
        own(3, values.at[me], out_values.at[me]),
    ]
    loads = {}
    for i, offset in enumerate(one_link + two_links):
        f, n = peers[offset]
        block = f * near + n
        loads[offset] = own(len(local) + i, keys.at[block], held_keys.at[block])
        loads[offset].start()

    barrier = pltpu.get_barrier_semaphore()
    for offset in one_link + two_links:
        greet = jnp.logical_or(
            jnp.logical_and(role == ROOT, roles[offset] != END),
            jnp.logical_or(
                jnp.logical_and(role == SIDE, roles[offset] != SIDE),
                jnp.logical_and(role == END, roles[offset] == END),
            ),
        )

        @pl.when(greet)
        def _(device=peers[offset]):
            pl.semaphore_signal(barrier, inc=1, device_id=place_of(device), device_id_type=MESH)

    local[2].start()
    sends = {}
    for i, (source, target) in enumerate(((held_keys, landed), (values, out_values))):
        for offset in offsets:
            f, n = peers[offset]
            sends[i, offset] = pltpu.make_async_remote_copy(
                src_ref=source.at[f * near + n],
                dst_ref=target.at[me],
                send_sem=send_sem.at[i, offsets.index(offset)],
                recv_sem=recv_sem.at[i, offsets.index(offset)],
                device_id=place_of((f, n)),
                device_id_type=MESH,
            )

    def tell(chosen):
        for offset in one_link + two_links:

            @pl.when(chosen(roles[offset]))
            def _(device=peers[offset]):
                pl.semaphore_signal(ready, inc=1, device_id=place_of(device), device_id_type=MESH)

    def send_keys(offset):
        loads[offset].wait()
        sends[0, offset].start()

    @pl.when(role == SIDE)
    def _():
        pl.semaphore_wait(barrier, roots)
        for offset in one_link:
            pl.when(roles[offset] == ROOT)(functools.partial(send_keys, offset))
        pl.semaphore_wait(ready, ends)
        tell(lambda other: other != SIDE)
        for offset in one_link:
            pl.when(roles[offset] != ROOT)(functools.partial(send_keys, offset))

    @pl.when(role != SIDE)
    def _():
        pl.semaphore_wait(barrier, jnp.where(role == ROOT, roots, ends) - 1 + sides)

        @pl.when(role == END)
        def _():
            tell(lambda other: other == SIDE)

        for offset in one_link:
            send_keys(offset)
        pl.semaphore_wait(ready, sides)

    for offset in two_links:
        send_keys(offset)
    for offset in two_links + one_link:
        sends[1, offset].start()

    for copy in (local[0], local[1], local[3]):
        copy.start()
    for copy in local[:3]:
        copy.wait()

    @pl.loop(0, angles.shape[1] // LANES)
    def _(step):
        start = pl.multiple_of(step * LANES, LANES)
        cosine, sine = cosine_and_sine(angles[:, pl.ds(start, LANES)])
        gain_row = gains[...]
        turn_same = jnp.concatenate([cosine, cosine], axis=0).T * gain_row
        turn_other = jnp.concatenate([-sine, sine], axis=0).T * pltpu.roll(
            gain_row, LANES // 2, 1
        )
        for head in range(heads):
            place = pl.ds(start * heads + head, LANES, stride=heads)
            cosines[place, :] = turn_same
            sines[place, :] = turn_other

    def turn_block(blocks, slot, largest):
        @functools.partial(lax.fori_loop, 0, rows // BLOCK, init_val=largest)
        def result(step, most):
            start = pl.multiple_of(step * BLOCK, BLOCK)
            place = pl.ds(pl.multiple_of(slot * rows + start, BLOCK), BLOCK)
            x = blocks[slot, pl.ds(start, BLOCK), :].astype(jnp.float32)
            mean = jnp.sum(x * x, axis=-1, keepdims=True) * (1.0 / LANES)
            scaled = x * cosines[place, :] + pltpu.roll(x, LANES // 2, 1) * sines[place, :]
            scaled = scaled * lax.rsqrt(mean + 1e-06)
            turned[place, :] = scaled
            return jnp.maximum(
                most, jnp.max(jnp.abs(scaled).reshape(-1, SUBLANES, LANES), axis=0)
            )

        return result

    most = jnp.zeros((SUBLANES, LANES), jnp.float32)
    most = turn_block(held_keys, me, most)
    for offset in one_link + two_links:
        f, n = peers[offset]
        sends[0, offset].wait_recv()
        most = turn_block(landed, f * near + n, most)
    scale = most[:heads]
    for row in range(heads, SUBLANES, heads):
        scale = jnp.maximum(scale, most[row : row + heads])
    out_scale[...] = scale
    inverse = jnp.concatenate([1.0 / scale] * (SUBLANES // heads), axis=0)[None]

    @pl.loop(0, members * rows // BLOCK)
    def _(step):
        place = pl.ds(pl.multiple_of(step * BLOCK, BLOCK), BLOCK)
        wide = turned[place, :].reshape(-1, SUBLANES, LANES) * inverse
        out_keys[place, :] = wide.reshape(BLOCK, LANES).astype(out_keys.dtype)

    local[3].wait()
    for offset in offsets:
        sends[1, offset].wait_recv()
    for send in sends.values():
        send.wait_send()


def hold(x):
    return pltpu.with_memory_space_constraint(x, pltpu.HBM)


def write_out(*refs):
    count = len(refs) // 2
    sources, targets, sems = refs[:count], refs[count : 2 * count], refs[-1]
    copies = [
        pltpu.make_async_copy(source, target, sems.at[i])
        for i, (source, target) in enumerate(zip(sources, targets))
    ]
    for copy in copies:
        copy.start()
    for copy in copies:
        copy.wait()


def shards(far, near, raw_keys, raw_values, turn_angle, key_gain):
    batch, length, heads, size = raw_keys.shape
    members = far * near
    assert batch == members and size == LANES and SUBLANES % heads == 0
    assert far > 2 and near > 1 and far & (far - 1) == 0 and near & (near - 1) == 0
    rows = length * heads
    offsets = [(f, n) for f in range(far) for n in range(near) if (f, n) != (0, 0)]
    offsets.sort(key=lambda o: (o[0] < 2 and o[1] == 0, o[1], o[0]))
    anywhere = pl.BlockSpec(memory_space=pl.ANY)
    inside = pl.BlockSpec(memory_space=pltpu.VMEM)
    results = pl.pallas_call(
        functools.partial(kernel, far, near, heads, offsets),
        out_shape=(
            pltpu.VMEM((members * rows, size), raw_keys.dtype),
            pltpu.VMEM((members, rows, size), raw_values.dtype),
            jax.ShapeDtypeStruct((heads, size), jnp.float32),
        ),
        in_specs=[anywhere] * 4,
        out_specs=(inside, inside, inside),
        scratch_shapes=[
            pltpu.VMEM((members, rows, size), raw_keys.dtype),
            pltpu.VMEM((members, rows, size), raw_keys.dtype),
            pltpu.VMEM((members * rows, size), jnp.float32),
            pltpu.VMEM((members * rows, size), jnp.float32),
            pltpu.VMEM((members * rows, size), jnp.float32),
            pltpu.VMEM((size // 2, members * length), jnp.float32),
            pltpu.VMEM((1, size), jnp.float32),
            pltpu.SemaphoreType.DMA((2, len(offsets))),
            pltpu.SemaphoreType.DMA((2, len(offsets))),
            pltpu.SemaphoreType.DMA((4 + len(offsets),)),
            pltpu.SemaphoreType.REGULAR,
        ],
        compiler_params=pltpu.CompilerParams(
            collective_id=0, has_side_effects=True, vmem_limit_bytes=32 * 1024 * 1024
        ),
        name="move_and_turn",
    )(
        hold(raw_keys.reshape(batch, rows, size)),
        hold(raw_values.reshape(batch, rows, size)),
        hold(turn_angle.T),
        hold(key_gain.reshape(1, size)),
    )
    narrow_keys, moved_values, key_scale = pl.pallas_call(
        write_out,
        out_shape=tuple(pltpu.HBM(r.shape, r.dtype) for r in results),
        in_specs=[anywhere] * len(results),
        out_specs=(anywhere,) * len(results),
        scratch_shapes=[pltpu.SemaphoreType.DMA((len(results),))],
        compiler_params=pltpu.CompilerParams(vmem_limit_bytes=2 * 1024 * 1024),
        name="write_out",
    )(*results)
    whole = (1, members * length, heads, size)
    return narrow_keys.reshape(whole), moved_values.reshape(whole), key_scale[None]


def solution(mesh):
    in_specs = (
        P(None, ("farcp", "nearcp"), "heads", None),
        P(None, ("farcp", "nearcp"), "heads", None),
        P(),
        P(),
    )
    out_specs = (
        P(("farcp", "nearcp"), None, "heads", None),
        P(("farcp", "nearcp"), None, "heads", None),
        P(("farcp", "nearcp"), "heads", None),
    )
    body = functools.partial(shards, mesh.shape["farcp"], mesh.shape["nearcp"])
    return jax.shard_map(body, mesh=mesh, in_specs=in_specs, out_specs=out_specs, check_vma=False)
```

```python
import functools

import jax
import jax.numpy as jnp
from jax import lax
from jax.experimental import pallas as pl
from jax.experimental.pallas import tpu as pltpu
from jax.sharding import PartitionSpec as P

MESH = pl.DeviceIdType.MESH
LANES = 128
SUBLANES = 8
BLOCK = 128
ROOT, SIDE, END = 0, 1, 2
SINE = (1.0, -0.1666666716337204, 0.008333330973982811, -0.00019840861205011606,
        2.752528644123231e-06, -2.3889498379503493e-08)
COSINE = (1.0, -0.5, 0.0416666679084301, -0.0013888884568586946, 2.4801040126476437e-05,
          -2.752468617472914e-07, 1.9907717696554528e-09)


def polynomial(coefficients, z):
    total = jnp.full_like(z, coefficients[-1])
    for coefficient in coefficients[-2::-1]:
        total = total * z + coefficient
    return total


def cosine_and_sine(angle):
    y = (1.57079637 - jnp.abs(angle)) - 4.371139e-08
    z = y * y
    sine = polynomial(COSINE, z)
    return y * polynomial(SINE, z), jnp.where(angle < 0, -sine, sine)


def partner(index, offset, size):
    result, bit = 0, 1
    while bit < size:
        digit = (index // bit) % 2
        result = result + ((digit + 1) % 2 if offset & bit else digit) * bit
        bit *= 2
    return result


def role_of(far_index, near_index):
    return jnp.where(far_index < 2, 0, 1) + jnp.where(near_index == 0, 0, 1)


def place_of(device):
    return {"farcp": device[0], "nearcp": device[1]}


def kernel(far, near, heads, offsets, keys, values, angle, gain, out_keys, out_values, out_scale,
           landed, held_keys, turned, cosines, sines, angles, gains, send_sem, recv_sem, local_sem, ready):
    members, rows, _ = landed.shape
    far_index, near_index = lax.axis_index("farcp"), lax.axis_index("nearcp")
    me = far_index * near + near_index
    one_link = [o for o in offsets if o[0] < 2 or o[1] == 0]
    two_links = [o for o in offsets if o not in one_link]
    peers = {
        (f, n): (partner(far_index, f, far), partner(near_index, n, near)) for f, n in offsets
    }
    role, roles = role_of(far_index, near_index), {o: role_of(*peers[o]) for o in offsets}
    roots, sides, ends = 2, 2 * (near - 1) + far - 2, (far - 2) * (near - 1)

    def own(i, source, target):
        return pltpu.make_async_copy(source, target, local_sem.at[i])

    local = [
        own(0, angle, angles),
        own(1, gain, gains),
        own(2, keys.at[me], held_keys.at[me]),
        own(3, values.at[me], out_values.at[me]),
    ]
    head = rows // 4
    first = ((2, 0), (0, 1))
    pieces = {o: (pl.ds(0, rows),) for o in one_link + two_links}
    for offset in first:
        pieces[offset] = (pl.ds(0, head), pl.ds(head, rows - head))

    def send(i, source, target, offset, place):
        f, n = peers[offset]
        return pltpu.make_async_remote_copy(
            src_ref=source.at[f * near + n, place],
            dst_ref=target.at[me, place],
            send_sem=send_sem.at[i, offsets.index(offset)],
            recv_sem=recv_sem.at[i, offsets.index(offset)],
            device_id=place_of((f, n)),
            device_id_type=MESH,
        )

    sends, loads = {}, {}
    for i, (source, target) in enumerate(((held_keys, landed), (values, out_values))):
        for offset in offsets:
            sends[i, offset] = send(i, source, target, offset, pl.ds(0, rows))
    for offset in one_link + two_links:
        f, n = peers[offset]
        for part, piece in enumerate(pieces[offset]):
            place = (f * near + n, piece)
            loads[offset, part] = own(len(local) + len(loads), keys.at[place], held_keys.at[place])

    barrier = pltpu.get_barrier_semaphore()
    for offset in one_link + two_links:
        greet = jnp.logical_or(
            jnp.logical_and(role == ROOT, roles[offset] != END),
            jnp.logical_and(role == SIDE, roles[offset] != SIDE),
        )

        @pl.when(greet)
        def _(device=peers[offset]):
            pl.semaphore_signal(barrier, inc=1, device_id=place_of(device), device_id_type=MESH)

    straight = {o: jnp.logical_and(role == SIDE, roles[o] == ROOT) for o in one_link}

    @pl.when(role == SIDE)
    def _():
        pl.semaphore_wait(barrier, roots)
        for offset in sorted(one_link, key=lambda o: -o[0]):
            pl.when(straight[offset])(send(0, keys, landed, offset, pl.ds(0, rows)).start)

    for offset, part in sorted(loads, key=lambda at: (at[0] not in first, at[1])):
        load = loads[offset, part].start
        if offset in straight:
            pl.when(jnp.logical_not(straight[offset]))(load)
        else:
            load()
    local[2].start()

    def tell(chosen):
        for offset in one_link + two_links:

            @pl.when(chosen(roles[offset]))
            def _(device=peers[offset]):
                pl.semaphore_signal(ready, inc=1, device_id=place_of(device), device_id_type=MESH)

    def send_keys(offset):
        for part, place in enumerate(pieces[offset]):
            loads[offset, part].wait()
            send(0, held_keys, landed, offset, place).start()

    @pl.when(role == SIDE)
    def _():
        pl.semaphore_wait(ready, ends)
        for offset in one_link:
            pl.when(roles[offset] == END)(functools.partial(send_keys, offset))
        tell(lambda other: other != SIDE)
        for offset in one_link:
            pl.when(roles[offset] == SIDE)(functools.partial(send_keys, offset))

    @pl.when(role != SIDE)
    def _():
        pl.semaphore_wait(barrier, jnp.where(role == ROOT, roots - 1, 0) + sides)

        @pl.when(role == END)
        def _():
            tell(lambda other: other == SIDE)

        for offset in one_link:
            pl.when(roles[offset] == SIDE)(functools.partial(send_keys, offset))
        pl.semaphore_wait(ready, sides)
        for offset in one_link:
            pl.when(roles[offset] != SIDE)(functools.partial(send_keys, offset))

    for offset in two_links:
        send_keys(offset)
    for offset in two_links + one_link:
        sends[1, offset].start()

    for copy in (local[0], local[1], local[3]):
        copy.start()
    for copy in local[:3]:
        copy.wait()

    @pl.loop(0, angles.shape[1] // LANES)
    def _(step):
        start = pl.multiple_of(step * LANES, LANES)
        cosine, sine = cosine_and_sine(angles[:, pl.ds(start, LANES)])
        gain_row = gains[...]
        turn_same = jnp.concatenate([cosine, cosine], axis=0).T * gain_row
        turn_other = jnp.concatenate([-sine, sine], axis=0).T * pltpu.roll(
            gain_row, LANES // 2, 1
        )
        for head in range(heads):
            place = pl.ds(start * heads + head, LANES, stride=heads)
            cosines[place, :] = turn_same
            sines[place, :] = turn_other

    def turn_block(blocks, slot, largest):
        @functools.partial(lax.fori_loop, 0, rows // BLOCK, init_val=largest)
        def result(step, most):
            start = pl.multiple_of(step * BLOCK, BLOCK)
            place = pl.ds(pl.multiple_of(slot * rows + start, BLOCK), BLOCK)
            x = blocks[slot, pl.ds(start, BLOCK), :].astype(jnp.float32)
            mean = jnp.sum(x * x, axis=-1, keepdims=True) * (1.0 / LANES)
            scaled = x * cosines[place, :] + pltpu.roll(x, LANES // 2, 1) * sines[place, :]
            scaled = scaled * lax.rsqrt(mean + 1e-06)
            turned[place, :] = scaled
            return jnp.maximum(
                most, jnp.max(jnp.abs(scaled).reshape(-1, SUBLANES, LANES), axis=0)
            )

        return result

    most = jnp.zeros((SUBLANES, LANES), jnp.float32)
    most = turn_block(held_keys, me, most)
    for offset in one_link + two_links:
        f, n = peers[offset]
        sends[0, offset].wait_recv()
        most = turn_block(landed, f * near + n, most)
    scale = most[:heads]
    for row in range(heads, SUBLANES, heads):
        scale = jnp.maximum(scale, most[row : row + heads])
    out_scale[...] = scale
    inverse = jnp.concatenate([1.0 / scale] * (SUBLANES // heads), axis=0)[None]

    @pl.loop(0, members * rows // BLOCK)
    def _(step):
        place = pl.ds(pl.multiple_of(step * BLOCK, BLOCK), BLOCK)
        wide = turned[place, :].reshape(-1, SUBLANES, LANES) * inverse
        out_keys[place, :] = wide.reshape(BLOCK, LANES).astype(out_keys.dtype)

    local[3].wait()
    for offset in offsets:
        sends[1, offset].wait_recv()
    for sent in sends.values():
        sent.wait_send()


def hold(x):
    return pltpu.with_memory_space_constraint(x, pltpu.HBM)


def write_out(*refs):
    count = len(refs) // 2
    sources, targets, sems = refs[:count], refs[count : 2 * count], refs[-1]
    copies = [
        pltpu.make_async_copy(source, target, sems.at[i])
        for i, (source, target) in enumerate(zip(sources, targets))
    ]
    for copy in copies:
        copy.start()
    for copy in copies:
        copy.wait()


def shards(far, near, raw_keys, raw_values, turn_angle, key_gain):
    batch, length, heads, size = raw_keys.shape
    members = far * near
    assert batch == members and size == LANES and SUBLANES % heads == 0
    assert far > 2 and near > 1 and far & (far - 1) == 0 and near & (near - 1) == 0
    rows = length * heads
    offsets = [(f, n) for f in range(far) for n in range(near) if (f, n) != (0, 0)]
    offsets.sort(key=lambda o: (o[0] < 2 and o[1] == 0, o[1], o[0]))
    anywhere = pl.BlockSpec(memory_space=pl.ANY)
    inside = pl.BlockSpec(memory_space=pltpu.VMEM)
    results = pl.pallas_call(
        functools.partial(kernel, far, near, heads, offsets),
        out_shape=(
            pltpu.VMEM((members * rows, size), raw_keys.dtype),
            pltpu.VMEM((members, rows, size), raw_values.dtype),
            jax.ShapeDtypeStruct((heads, size), jnp.float32),
        ),
        in_specs=[anywhere] * 4,
        out_specs=(inside, inside, inside),
        scratch_shapes=[
            pltpu.VMEM((members, rows, size), raw_keys.dtype),
            pltpu.VMEM((members, rows, size), raw_keys.dtype),
            pltpu.VMEM((members * rows, size), jnp.float32),
            pltpu.VMEM((members * rows, size), jnp.float32),
            pltpu.VMEM((members * rows, size), jnp.float32),
            pltpu.VMEM((size // 2, members * length), jnp.float32),
            pltpu.VMEM((1, size), jnp.float32),
            pltpu.SemaphoreType.DMA((2, len(offsets))),
            pltpu.SemaphoreType.DMA((2, len(offsets))),
            pltpu.SemaphoreType.DMA((6 + len(offsets),)),
            pltpu.SemaphoreType.REGULAR,
        ],
        compiler_params=pltpu.CompilerParams(
            collective_id=0, has_side_effects=True, vmem_limit_bytes=32 * 1024 * 1024
        ),
        name="move_and_turn",
    )(
        hold(raw_keys.reshape(batch, rows, size)),
        hold(raw_values.reshape(batch, rows, size)),
        hold(turn_angle.T),
        hold(key_gain.reshape(1, size)),
    )
    narrow_keys, moved_values, key_scale = pl.pallas_call(
        write_out,
        out_shape=tuple(pltpu.HBM(r.shape, r.dtype) for r in results),
        in_specs=[anywhere] * len(results),
        out_specs=(anywhere,) * len(results),
        scratch_shapes=[pltpu.SemaphoreType.DMA((len(results),))],
        compiler_params=pltpu.CompilerParams(vmem_limit_bytes=2 * 1024 * 1024),
        name="write_out",
    )(*results)
    whole = (1, members * length, heads, size)
    return narrow_keys.reshape(whole), moved_values.reshape(whole), key_scale[None]


def solution(mesh):
    in_specs = (
        P(None, ("farcp", "nearcp"), "heads", None),
        P(None, ("farcp", "nearcp"), "heads", None),
        P(),
        P(),
    )
    out_specs = (
        P(("farcp", "nearcp"), None, "heads", None),
        P(("farcp", "nearcp"), None, "heads", None),
        P(("farcp", "nearcp"), "heads", None),
    )
    body = functools.partial(shards, mesh.shape["farcp"], mesh.shape["nearcp"])
    return jax.shard_map(body, mesh=mesh, in_specs=in_specs, out_specs=out_specs, check_vma=False)
```

```python
import functools

import jax
import jax.numpy as jnp
from jax import lax
from jax.experimental import pallas as pl
from jax.experimental.pallas import tpu as pltpu
from jax.sharding import PartitionSpec as P

MESH = pl.DeviceIdType.MESH
LANES = 128
SUBLANES = 8
BLOCK = 128
ROOT, SIDE, END = 0, 1, 2
SINE = (1.0, -0.1666666716337204, 0.008333330973982811, -0.00019840861205011606,
        2.752528644123231e-06, -2.3889498379503493e-08)
COSINE = (1.0, -0.5, 0.0416666679084301, -0.0013888884568586946, 2.4801040126476437e-05,
          -2.752468617472914e-07, 1.9907717696554528e-09)


def polynomial(coefficients, z):
    total = jnp.full_like(z, coefficients[-1])
    for coefficient in coefficients[-2::-1]:
        total = total * z + coefficient
    return total


def cosine_and_sine(angle):
    y = (1.57079637 - jnp.abs(angle)) - 4.371139e-08
    z = y * y
    sine = polynomial(COSINE, z)
    return y * polynomial(SINE, z), jnp.where(angle < 0, -sine, sine)


def partner(index, offset, size):
    result, bit = 0, 1
    while bit < size:
        digit = (index // bit) % 2
        result = result + ((digit + 1) % 2 if offset & bit else digit) * bit
        bit *= 2
    return result


def role_of(far_index, near_index):
    return jnp.where(far_index < 2, 0, 1) + jnp.where(near_index == 0, 0, 1)


def place_of(device):
    return {"farcp": device[0], "nearcp": device[1]}


def kernel(far, near, heads, offsets, keys, values, angle, gain, out_keys, out_values, out_scale,
           landed, held_keys, turned, cosines, sines, angles, gains, send_sem, recv_sem, local_sem,
           ready, link):
    members, rows, _ = landed.shape
    far_index, near_index = lax.axis_index("farcp"), lax.axis_index("nearcp")
    me = far_index * near + near_index
    one_link = [o for o in offsets if o[0] < 2 or o[1] == 0]
    two_links = [o for o in offsets if o not in one_link]
    peers = {
        (f, n): (partner(far_index, f, far), partner(near_index, n, near)) for f, n in offsets
    }
    role, roles = role_of(far_index, near_index), {o: role_of(*peers[o]) for o in offsets}
    core = far_index % 2
    odd, mate = core == 1, (far_index + 1 - 2 * core, near_index)
    roots = [(f, 0) for f in range(2)]
    sides = [(f, n) for f in range(2) for n in range(1, near)] + [(f, 0) for f in range(2, far)]
    ends = [(f, n) for f in range(2, far) for n in range(1, near)]

    def own(i, source, target):
        return pltpu.make_async_copy(source, target, local_sem.at[i])

    local = [
        own(0, angle, angles),
        own(1, gain, gains),
        own(2, keys.at[me], held_keys.at[me]),
        own(3, values.at[me], out_values.at[me]),
    ]
    head = rows // 4
    first = ((2, 0), (0, 1))
    pieces = {o: (pl.ds(0, rows),) for o in one_link + two_links}
    for offset in first:
        pieces[offset] = (pl.ds(0, head), pl.ds(head, rows - head))

    def send(i, source, target, offset, place):
        f, n = peers[offset]
        return pltpu.make_async_remote_copy(
            src_ref=source.at[f * near + n, place],
            dst_ref=target.at[me, place],
            send_sem=send_sem.at[i, offset[0] * near + offset[1]],
            recv_sem=recv_sem.at[i, offset[0] * near + offset[1]],
            device_id=place_of((f, n)),
            device_id_type=MESH,
        )

    sends, loads = {}, {}
    for i, (source, target) in enumerate(((held_keys, landed), (values, out_values))):
        for offset in offsets:
            sends[i, offset] = send(i, source, target, offset, pl.ds(0, rows))
    for offset in one_link + two_links:
        f, n = peers[offset]
        for part, piece in enumerate(pieces[offset]):
            place = (f * near + n, piece)
            loads[offset, part] = own(len(local) + len(loads), keys.at[place], held_keys.at[place])

    def tell(semaphore, devices):
        for device in devices:
            pl.semaphore_signal(
                semaphore, inc=1, device_id=place_of(device), device_id_type=MESH
            )

    def send_straight():
        for root, far_step in ((1 - core, far_index + 1 - core), (core, far_index - core)):
            pltpu.make_async_remote_copy(
                src_ref=keys.at[root * near],
                dst_ref=landed.at[me],
                send_sem=send_sem.at[0, far_step * near + near_index],
                recv_sem=recv_sem.at[0, far_step * near + near_index],
                device_id=place_of((root, 0)),
                device_id_type=MESH,
            ).start()

    barrier = pltpu.get_barrier_semaphore()

    @pl.when(role == SIDE)
    def _():
        @pl.when(odd)
        def _():
            tell(barrier, roots)

        tell(barrier, ends)

        @pl.when(odd)
        def _():
            tell(barrier, [mate])
            pl.semaphore_wait(barrier, len(roots))
            send_straight()

    @pl.when(role == ROOT)
    def _():
        tell(barrier, [mate] + [d for d in sides if d[0] % 2 == 1])

    @pl.when(role == END)
    def _():
        tell(barrier, [d for d in sides if d[0] % 2 == 0])

    straight = {o: jnp.logical_and(role == SIDE, roles[o] == ROOT) for o in one_link}
    for offset, part in sorted(loads, key=lambda at: (at[0] not in first, at[1])):
        load = loads[offset, part].start
        if offset in straight:
            pl.when(jnp.logical_not(straight[offset]))(load)
        else:
            load()
    local[2].start()

    def send_keys(offset):
        for part, place in enumerate(pieces[offset]):
            loads[offset, part].wait()
            send(0, held_keys, landed, offset, place).start()

    def send_to(chosen):
        for offset in one_link:
            pl.when(chosen(roles[offset]))(functools.partial(send_keys, offset))

    @pl.when(role == SIDE)
    def _():
        @pl.when(odd)
        def _():
            pl.semaphore_wait(link, 1)

        @pl.when(jnp.logical_not(odd))
        def _():
            pl.semaphore_wait(barrier, len(ends) + 1)

        tell(link, [mate])

        @pl.when(jnp.logical_not(odd))
        def _():
            pl.semaphore_wait(link, 1)
            send_straight()

        send_to(lambda other: other == END)

        tell(ready, roots + ends)
        pl.semaphore_wait(ready, 1)
        send_to(lambda other: other == SIDE)

    @pl.when(role == ROOT)
    def _():
        pl.semaphore_wait(barrier, len(roots) - 1 + len(sides) // 2)
        for wanted in (1, 0):
            for offset in one_link:
                chosen = jnp.logical_and(roles[offset] == SIDE, peers[offset][0] % 2 == wanted)
                pl.when(chosen)(functools.partial(send_keys, offset))
            if wanted:
                pl.semaphore_wait(ready, len(sides))
                tell(ready, [(d[0] + core, d[1]) for d in sides if d[0] % 2 == 0])
        send_to(lambda other: other == ROOT)

    @pl.when(role == END)
    def _():
        pl.semaphore_wait(barrier, len(sides))
        send_to(lambda other: other == SIDE)
        pl.semaphore_wait(ready, len(sides))
        send_to(lambda other: other == END)

    for offset in two_links:
        send_keys(offset)
    inner = jnp.logical_and(role == SIDE, near_index == 0)
    across = [o for o in one_link if o[0] >= 2]
    for offset in across:
        pl.when(inner)(sends[1, offset].start)
    for offset in two_links:
        sends[1, offset].start()
    for offset in across:
        pl.when(jnp.logical_not(inner))(sends[1, offset].start)
    for offset in one_link:
        if offset not in across:
            sends[1, offset].start()

    for copy in (local[0], local[1], local[3]):
        copy.start()
    for copy in local[:3]:
        copy.wait()

    @pl.loop(0, angles.shape[1] // LANES)
    def _(step):
        start = pl.multiple_of(step * LANES, LANES)
        cosine, sine = cosine_and_sine(angles[:, pl.ds(start, LANES)])
        gain_row = gains[...]
        turn_same = jnp.concatenate([cosine, cosine], axis=0).T * gain_row
        turn_other = jnp.concatenate([-sine, sine], axis=0).T * pltpu.roll(
            gain_row, LANES // 2, 1
        )
        for head in range(heads):
            place = pl.ds(start * heads + head, LANES, stride=heads)
            cosines[place, :] = turn_same
            sines[place, :] = turn_other

    def turn_block(blocks, slot, largest):
        @functools.partial(lax.fori_loop, 0, rows // BLOCK, init_val=largest)
        def result(step, most):
            start = pl.multiple_of(step * BLOCK, BLOCK)
            place = pl.ds(pl.multiple_of(slot * rows + start, BLOCK), BLOCK)
            x = blocks[slot, pl.ds(start, BLOCK), :].astype(jnp.float32)
            mean = jnp.sum(x * x, axis=-1, keepdims=True) * (1.0 / LANES)
            scaled = x * cosines[place, :] + pltpu.roll(x, LANES // 2, 1) * sines[place, :]
            scaled = scaled * lax.rsqrt(mean + 1e-06)
            turned[place, :] = scaled
            return jnp.maximum(
                most, jnp.max(jnp.abs(scaled).reshape(-1, SUBLANES, LANES), axis=0)
            )

        return result

    most = jnp.zeros((SUBLANES, LANES), jnp.float32)
    most = turn_block(held_keys, me, most)
    for offset in sorted(one_link + two_links, key=lambda o: o[0] == 1 and o[1] > 0):
        f, n = peers[offset]
        sends[0, offset].wait_recv()
        most = turn_block(landed, f * near + n, most)
    scale = most[:heads]
    for row in range(heads, SUBLANES, heads):
        scale = jnp.maximum(scale, most[row : row + heads])
    out_scale[...] = scale
    inverse = jnp.concatenate([1.0 / scale] * (SUBLANES // heads), axis=0)[None]

    @pl.loop(0, members * rows // BLOCK)
    def _(step):
        place = pl.ds(pl.multiple_of(step * BLOCK, BLOCK), BLOCK)
        wide = turned[place, :].reshape(-1, SUBLANES, LANES) * inverse
        out_keys[place, :] = wide.reshape(BLOCK, LANES).astype(out_keys.dtype)

    local[3].wait()
    for offset in offsets:
        sends[1, offset].wait_recv()
    for sent in sends.values():
        sent.wait_send()


def hold(x):
    return pltpu.with_memory_space_constraint(x, pltpu.HBM)


def write_out(*refs):
    count = len(refs) // 2
    sources, targets, sems = refs[:count], refs[count : 2 * count], refs[-1]
    copies = [
        pltpu.make_async_copy(source, target, sems.at[i])
        for i, (source, target) in enumerate(zip(sources, targets))
    ]
    for copy in copies:
        copy.start()
    for copy in copies:
        copy.wait()


def shards(far, near, raw_keys, raw_values, turn_angle, key_gain):
    batch, length, heads, size = raw_keys.shape
    members = far * near
    assert batch == members and size == LANES and SUBLANES % heads == 0
    assert far > 2 and near > 1 and far & (far - 1) == 0 and near & (near - 1) == 0
    rows = length * heads
    offsets = [(f, n) for f in range(far) for n in range(near) if (f, n) != (0, 0)]
    offsets.sort(key=lambda o: (o[0] < 2 and o[1] == 0, o[1], o[0]))
    anywhere = pl.BlockSpec(memory_space=pl.ANY)
    inside = pl.BlockSpec(memory_space=pltpu.VMEM)
    results = pl.pallas_call(
        functools.partial(kernel, far, near, heads, offsets),
        out_shape=(
            pltpu.VMEM((members * rows, size), raw_keys.dtype),
            pltpu.VMEM((members, rows, size), raw_values.dtype),
            jax.ShapeDtypeStruct((heads, size), jnp.float32),
        ),
        in_specs=[anywhere] * 4,
        out_specs=(inside, inside, inside),
        scratch_shapes=[
            pltpu.VMEM((members, rows, size), raw_keys.dtype),
            pltpu.VMEM((members, rows, size), raw_keys.dtype),
            pltpu.VMEM((members * rows, size), jnp.float32),
            pltpu.VMEM((members * rows, size), jnp.float32),
            pltpu.VMEM((members * rows, size), jnp.float32),
            pltpu.VMEM((size // 2, members * length), jnp.float32),
            pltpu.VMEM((1, size), jnp.float32),
            pltpu.SemaphoreType.DMA((2, members)),
            pltpu.SemaphoreType.DMA((2, members)),
            pltpu.SemaphoreType.DMA((6 + len(offsets),)),
            pltpu.SemaphoreType.REGULAR,
            pltpu.SemaphoreType.REGULAR,
        ],
        compiler_params=pltpu.CompilerParams(
            collective_id=0, has_side_effects=True, vmem_limit_bytes=32 * 1024 * 1024
        ),
        name="move_and_turn",
    )(
        hold(raw_keys.reshape(batch, rows, size)),
        hold(raw_values.reshape(batch, rows, size)),
        hold(turn_angle.T),
        hold(key_gain.reshape(1, size)),
    )
    narrow_keys, moved_values, key_scale = pl.pallas_call(
        write_out,
        out_shape=tuple(pltpu.HBM(r.shape, r.dtype) for r in results),
        in_specs=[anywhere] * len(results),
        out_specs=(anywhere,) * len(results),
        scratch_shapes=[pltpu.SemaphoreType.DMA((len(results),))],
        compiler_params=pltpu.CompilerParams(vmem_limit_bytes=2 * 1024 * 1024),
        name="write_out",
    )(*results)
    whole = (1, members * length, heads, size)
    return narrow_keys.reshape(whole), moved_values.reshape(whole), key_scale[None]


def solution(mesh):
    in_specs = (
        P(None, ("farcp", "nearcp"), "heads", None),
        P(None, ("farcp", "nearcp"), "heads", None),
        P(),
        P(),
    )
    out_specs = (
        P(("farcp", "nearcp"), None, "heads", None),
        P(("farcp", "nearcp"), None, "heads", None),
        P(("farcp", "nearcp"), "heads", None),
    )
    body = functools.partial(shards, mesh.shape["farcp"], mesh.shape["nearcp"])
    return jax.shard_map(body, mesh=mesh, in_specs=in_specs, out_specs=out_specs, check_vma=False)
```

```python
import functools

import jax
import jax.numpy as jnp
from jax import lax
from jax.experimental import pallas as pl
from jax.experimental.pallas import tpu as pltpu
from jax.sharding import PartitionSpec as P

MESH = pl.DeviceIdType.MESH
LANES = 128
SUBLANES = 8
BLOCK = 128
ROOT, SIDE, END = 0, 1, 2
SINE = (1.0, -0.1666666716337204, 0.008333330973982811, -0.00019840861205011606,
        2.752528644123231e-06, -2.3889498379503493e-08)
COSINE = (1.0, -0.5, 0.0416666679084301, -0.0013888884568586946, 2.4801040126476437e-05,
          -2.752468617472914e-07, 1.9907717696554528e-09)


def polynomial(coefficients, z):
    total = jnp.full_like(z, coefficients[-1])
    for coefficient in coefficients[-2::-1]:
        total = total * z + coefficient
    return total


def cosine_and_sine(angle):
    y = (1.57079637 - jnp.abs(angle)) - 4.371139e-08
    z = y * y
    sine = polynomial(COSINE, z)
    return y * polynomial(SINE, z), jnp.where(angle < 0, -sine, sine)


def partner(index, offset, size):
    result, bit = 0, 1
    while bit < size:
        digit = (index // bit) % 2
        result = result + ((digit + 1) % 2 if offset & bit else digit) * bit
        bit *= 2
    return result


def role_of(far_index, near_index):
    return jnp.where(far_index < 2, 0, 1) + jnp.where(near_index == 0, 0, 1)


def place_of(device):
    return {"farcp": device[0], "nearcp": device[1]}


def kernel(far, near, heads, offsets, keys, values, angle, gain, out_keys, out_values, out_scale,
           landed, held_keys, turned, cosines, sines, angles, gains, send_sem, recv_sem, local_sem,
           ready, link, more):
    members, rows, _ = landed.shape
    far_index, near_index = lax.axis_index("farcp"), lax.axis_index("nearcp")
    me = far_index * near + near_index
    one_link = [o for o in offsets if o[0] < 2 or o[1] == 0]
    two_links = [o for o in offsets if o not in one_link]
    peers = {
        (f, n): (partner(far_index, f, far), partner(near_index, n, near)) for f, n in offsets
    }
    role, roles = role_of(far_index, near_index), {o: role_of(*peers[o]) for o in offsets}
    core = far_index % 2
    odd, mate = core == 1, (far_index + 1 - 2 * core, near_index)
    roots = [(f, 0) for f in range(2)]
    sides = [(f, n) for f in range(2) for n in range(1, near)] + [(f, 0) for f in range(2, far)]
    ends = [(f, n) for f in range(2, far) for n in range(1, near)]

    def own(i, source, target):
        return pltpu.make_async_copy(source, target, local_sem.at[i])

    local = [
        own(0, angle, angles),
        own(1, gain, gains),
        own(2, keys.at[me], held_keys.at[me]),
        own(3, values.at[me], out_values.at[me]),
    ]
    head = rows // 4
    first = ((2, 0), (0, 1))
    pieces = {o: (pl.ds(0, rows),) for o in one_link + two_links}
    for offset in first:
        pieces[offset] = (pl.ds(0, head), pl.ds(head, rows - head))

    def send(i, source, target, offset, place):
        f, n = peers[offset]
        return pltpu.make_async_remote_copy(
            src_ref=source.at[f * near + n, place],
            dst_ref=target.at[me, place],
            send_sem=send_sem.at[i, offset[0] * near + offset[1]],
            recv_sem=recv_sem.at[i, offset[0] * near + offset[1]],
            device_id=place_of((f, n)),
            device_id_type=MESH,
        )

    sends, loads = {}, {}
    for i, (source, target) in enumerate(((held_keys, landed), (values, out_values))):
        for offset in offsets:
            sends[i, offset] = send(i, source, target, offset, pl.ds(0, rows))
    for offset in one_link + two_links:
        f, n = peers[offset]
        for part, piece in enumerate(pieces[offset]):
            place = (f * near + n, piece)
            loads[offset, part] = own(len(local) + len(loads), keys.at[place], held_keys.at[place])

    def tell(semaphore, devices):
        for device in devices:
            pl.semaphore_signal(
                semaphore, inc=1, device_id=place_of(device), device_id_type=MESH
            )

    def send_straight():
        for root, far_step in ((1 - core, far_index + 1 - core), (core, far_index - core)):
            pltpu.make_async_remote_copy(
                src_ref=keys.at[root * near],
                dst_ref=landed.at[me],
                send_sem=send_sem.at[0, far_step * near + near_index],
                recv_sem=recv_sem.at[0, far_step * near + near_index],
                device_id=place_of((root, 0)),
                device_id_type=MESH,
            ).start()

    barrier = pltpu.get_barrier_semaphore()

    @pl.when(role == SIDE)
    def _():
        @pl.when(odd)
        def _():
            tell(barrier, roots)

        tell(barrier, ends)

        @pl.when(odd)
        def _():
            tell(barrier, [mate])
            pl.semaphore_wait(barrier, len(roots))
            send_straight()

    @pl.when(role == ROOT)
    def _():
        tell(barrier, [mate] + [d for d in sides if d[0] % 2 == 1])

    @pl.when(role == END)
    def _():
        @pl.when(odd)
        def _():
            tell(barrier, [d for d in sides if d[0] % 2 == 0])

        @pl.when(jnp.logical_not(odd))
        def _():
            tell(barrier, [mate])

    straight = {o: jnp.logical_and(role == SIDE, roles[o] == ROOT) for o in one_link}
    for offset, part in sorted(loads, key=lambda at: (at[0] not in first, at[1])):
        load = loads[offset, part].start
        if offset in straight:
            pl.when(jnp.logical_not(straight[offset]))(load)
        else:
            load()
    local[2].start()

    def send_keys(offset):
        for part, place in enumerate(pieces[offset]):
            loads[offset, part].wait()
            send(0, held_keys, landed, offset, place).start()

    def send_to(other, *cores):
        for offset in one_link:
            chosen = roles[offset] == other
            for wanted in cores:
                chosen = jnp.logical_and(chosen, peers[offset][0] % 2 == wanted)
            pl.when(chosen)(functools.partial(send_keys, offset))

    @pl.when(role == SIDE)
    def _():
        @pl.when(odd)
        def _():
            pl.semaphore_wait(link, 1)

        @pl.when(jnp.logical_not(odd))
        def _():
            pl.semaphore_wait(barrier, len(ends) // 2 + 1)

        tell(link, [mate])
        send_to(END, 1)

        @pl.when(jnp.logical_not(odd))
        def _():
            pl.semaphore_wait(link, 1)
            send_straight()

        pl.semaphore_wait(more, len(ends) // 2)
        send_to(END, 0)
        tell(ready, roots + ends)
        pl.semaphore_wait(ready, 1)
        send_to(SIDE)

    @pl.when(role == ROOT)
    def _():
        pl.semaphore_wait(barrier, len(roots) - 1 + len(sides) // 2)
        send_to(SIDE, 1)
        pl.semaphore_wait(ready, len(sides))
        tell(ready, [(d[0] + core, d[1]) for d in sides if d[0] % 2 == 0])
        send_to(SIDE, 0)
        send_to(ROOT)

    @pl.when(role == END)
    def _():
        pl.semaphore_wait(barrier, len(sides) + core)
        pl.when(odd)(functools.partial(tell, more, sides))
        send_to(SIDE)
        pl.semaphore_wait(ready, len(sides))
        send_to(END)

    for offset in two_links:
        send_keys(offset)
    inner = jnp.logical_and(role == SIDE, near_index == 0)
    across = [o for o in one_link if o[0] >= 2]
    for offset in across:
        pl.when(inner)(sends[1, offset].start)
    for offset in two_links:
        sends[1, offset].start()
    for offset in across:
        pl.when(jnp.logical_not(inner))(sends[1, offset].start)
    for offset in one_link:
        if offset not in across:
            sends[1, offset].start()

    for copy in (local[0], local[1], local[3]):
        copy.start()
    for copy in local[:3]:
        copy.wait()

    @pl.loop(0, angles.shape[1] // LANES)
    def _(step):
        start = pl.multiple_of(step * LANES, LANES)
        cosine, sine = cosine_and_sine(angles[:, pl.ds(start, LANES)])
        gain_row = gains[...]
        turn_same = jnp.concatenate([cosine, cosine], axis=0).T * gain_row
        turn_other = jnp.concatenate([-sine, sine], axis=0).T * pltpu.roll(
            gain_row, LANES // 2, 1
        )
        for head in range(heads):
            place = pl.ds(start * heads + head, LANES, stride=heads)
            cosines[place, :] = turn_same
            sines[place, :] = turn_other

    def turn_block(blocks, slot, largest):
        @functools.partial(lax.fori_loop, 0, rows // BLOCK, init_val=largest)
        def result(step, most):
            start = pl.multiple_of(step * BLOCK, BLOCK)
            place = pl.ds(pl.multiple_of(slot * rows + start, BLOCK), BLOCK)
            x = blocks[slot, pl.ds(start, BLOCK), :].astype(jnp.float32)
            mean = jnp.sum(x * x, axis=-1, keepdims=True) * (1.0 / LANES)
            scaled = x * cosines[place, :] + pltpu.roll(x, LANES // 2, 1) * sines[place, :]
            scaled = scaled * lax.rsqrt(mean + 1e-06)
            turned[place, :] = scaled
            return jnp.maximum(
                most, jnp.max(jnp.abs(scaled).reshape(-1, SUBLANES, LANES), axis=0)
            )

        return result

    most = jnp.zeros((SUBLANES, LANES), jnp.float32)
    most = turn_block(held_keys, me, most)
    for offset in sorted(one_link + two_links, key=lambda o: o[0] == 1 and o[1] > 0):
        f, n = peers[offset]
        sends[0, offset].wait_recv()
        most = turn_block(landed, f * near + n, most)
    scale = most[:heads]
    for row in range(heads, SUBLANES, heads):
        scale = jnp.maximum(scale, most[row : row + heads])
    out_scale[...] = scale
    inverse = jnp.concatenate([1.0 / scale] * (SUBLANES // heads), axis=0)[None]

    @pl.loop(0, members * rows // BLOCK)
    def _(step):
        place = pl.ds(pl.multiple_of(step * BLOCK, BLOCK), BLOCK)
        wide = turned[place, :].reshape(-1, SUBLANES, LANES) * inverse
        out_keys[place, :] = wide.reshape(BLOCK, LANES).astype(out_keys.dtype)

    local[3].wait()
    for offset in offsets:
        sends[1, offset].wait_recv()
    for sent in sends.values():
        sent.wait_send()


def hold(x):
    return pltpu.with_memory_space_constraint(x, pltpu.HBM)


def write_out(*refs):
    count = len(refs) // 2
    sources, targets, sems = refs[:count], refs[count : 2 * count], refs[-1]
    copies = [
        pltpu.make_async_copy(source, target, sems.at[i])
        for i, (source, target) in enumerate(zip(sources, targets))
    ]
    for copy in copies:
        copy.start()
    for copy in copies:
        copy.wait()


def shards(far, near, raw_keys, raw_values, turn_angle, key_gain):
    batch, length, heads, size = raw_keys.shape
    members = far * near
    assert batch == members and size == LANES and SUBLANES % heads == 0
    assert far > 2 and near > 1 and far & (far - 1) == 0 and near & (near - 1) == 0
    rows = length * heads
    offsets = [(f, n) for f in range(far) for n in range(near) if (f, n) != (0, 0)]
    offsets.sort(key=lambda o: (o[0] < 2 and o[1] == 0, o[1], o[0]))
    anywhere = pl.BlockSpec(memory_space=pl.ANY)
    inside = pl.BlockSpec(memory_space=pltpu.VMEM)
    results = pl.pallas_call(
        functools.partial(kernel, far, near, heads, offsets),
        out_shape=(
            pltpu.VMEM((members * rows, size), raw_keys.dtype),
            pltpu.VMEM((members, rows, size), raw_values.dtype),
            jax.ShapeDtypeStruct((heads, size), jnp.float32),
        ),
        in_specs=[anywhere] * 4,
        out_specs=(inside, inside, inside),
        scratch_shapes=[
            pltpu.VMEM((members, rows, size), raw_keys.dtype),
            pltpu.VMEM((members, rows, size), raw_keys.dtype),
            pltpu.VMEM((members * rows, size), jnp.float32),
            pltpu.VMEM((members * rows, size), jnp.float32),
            pltpu.VMEM((members * rows, size), jnp.float32),
            pltpu.VMEM((size // 2, members * length), jnp.float32),
            pltpu.VMEM((1, size), jnp.float32),
            pltpu.SemaphoreType.DMA((2, members)),
            pltpu.SemaphoreType.DMA((2, members)),
            pltpu.SemaphoreType.DMA((6 + len(offsets),)),
            pltpu.SemaphoreType.REGULAR,
            pltpu.SemaphoreType.REGULAR,
            pltpu.SemaphoreType.REGULAR,
        ],
        compiler_params=pltpu.CompilerParams(
            collective_id=0, has_side_effects=True, vmem_limit_bytes=32 * 1024 * 1024
        ),
        name="move_and_turn",
    )(
        hold(raw_keys.reshape(batch, rows, size)),
        hold(raw_values.reshape(batch, rows, size)),
        hold(turn_angle.T),
        hold(key_gain.reshape(1, size)),
    )
    narrow_keys, moved_values, key_scale = pl.pallas_call(
        write_out,
        out_shape=tuple(pltpu.HBM(r.shape, r.dtype) for r in results),
        in_specs=[anywhere] * len(results),
        out_specs=(anywhere,) * len(results),
        scratch_shapes=[pltpu.SemaphoreType.DMA((len(results),))],
        compiler_params=pltpu.CompilerParams(vmem_limit_bytes=2 * 1024 * 1024),
        name="write_out",
    )(*results)
    whole = (1, members * length, heads, size)
    return narrow_keys.reshape(whole), moved_values.reshape(whole), key_scale[None]


def solution(mesh):
    in_specs = (
        P(None, ("farcp", "nearcp"), "heads", None),
        P(None, ("farcp", "nearcp"), "heads", None),
        P(),
        P(),
    )
    out_specs = (
        P(("farcp", "nearcp"), None, "heads", None),
        P(("farcp", "nearcp"), None, "heads", None),
        P(("farcp", "nearcp"), "heads", None),
    )
    body = functools.partial(shards, mesh.shape["farcp"], mesh.shape["nearcp"])
    return jax.shard_map(body, mesh=mesh, in_specs=in_specs, out_specs=out_specs, check_vma=False)
```

```python
import functools

import jax
import jax.numpy as jnp
from jax import lax
from jax.experimental import pallas as pl
from jax.experimental.pallas import tpu as pltpu
from jax.sharding import PartitionSpec as P

MESH = pl.DeviceIdType.MESH
LANES = 128
SUBLANES = 8
BLOCK = 128
ROOT, SIDE, END = 0, 1, 2
SINE = (1.0, -0.1666666716337204, 0.008333330973982811, -0.00019840861205011606,
        2.752528644123231e-06, -2.3889498379503493e-08)
COSINE = (1.0, -0.5, 0.0416666679084301, -0.0013888884568586946, 2.4801040126476437e-05,
          -2.752468617472914e-07, 1.9907717696554528e-09)


def polynomial(coefficients, z):
    total = jnp.full_like(z, coefficients[-1])
    for coefficient in coefficients[-2::-1]:
        total = total * z + coefficient
    return total


def cosine_and_sine(angle):
    y = (1.57079637 - jnp.abs(angle)) - 4.371139e-08
    z = y * y
    sine = polynomial(COSINE, z)
    return y * polynomial(SINE, z), jnp.where(angle < 0, -sine, sine)


def partner(index, offset, size):
    result, bit = 0, 1
    while bit < size:
        digit = (index // bit) % 2
        result = result + ((digit + 1) % 2 if offset & bit else digit) * bit
        bit *= 2
    return result


def role_of(far_index, near_index):
    return jnp.where(far_index < 2, 0, 1) + jnp.where(near_index == 0, 0, 1)


def place_of(device):
    return {"farcp": device[0], "nearcp": device[1]}


def kernel(far, near, heads, offsets, keys, values, angle, gain, out_keys, out_values, out_scale,
           landed, held_keys, turned, cosines, sines, angles, gains, send_sem, recv_sem, local_sem,
           ready, link, more):
    members, rows, _ = landed.shape
    far_index, near_index = lax.axis_index("farcp"), lax.axis_index("nearcp")
    me = far_index * near + near_index
    one_link = [o for o in offsets if o[0] < 2 or o[1] == 0]
    two_links = [o for o in offsets if o not in one_link]
    peers = {
        (f, n): (partner(far_index, f, far), partner(near_index, n, near)) for f, n in offsets
    }
    role, roles = role_of(far_index, near_index), {o: role_of(*peers[o]) for o in offsets}
    core = far_index % 2
    odd, mate = core == 1, (far_index + 1 - 2 * core, near_index)
    roots = [(f, 0) for f in range(2)]
    sides = [(f, n) for f in range(2) for n in range(1, near)] + [(f, 0) for f in range(2, far)]
    ends = [(f, n) for f in range(2, far) for n in range(1, near)]

    def own(i, source, target):
        return pltpu.make_async_copy(source, target, local_sem.at[i])

    local = [
        own(0, angle, angles),
        own(1, gain, gains),
        own(2, keys.at[me], held_keys.at[me]),
        own(3, values.at[me], out_values.at[me]),
    ]
    head = rows // 4
    first = ((2, 0), (0, 1))
    pieces = {o: (pl.ds(0, rows),) for o in one_link + two_links}
    for offset in first:
        pieces[offset] = (pl.ds(0, head), pl.ds(head, rows - head))

    def send(i, source, target, offset, place):
        f, n = peers[offset]
        return pltpu.make_async_remote_copy(
            src_ref=source.at[f * near + n, place],
            dst_ref=target.at[me, place],
            send_sem=send_sem.at[i, offset[0] * near + offset[1]],
            recv_sem=recv_sem.at[i, offset[0] * near + offset[1]],
            device_id=place_of((f, n)),
            device_id_type=MESH,
        )

    sends, loads = {}, {}
    for i, (source, target) in enumerate(((held_keys, landed), (values, out_values))):
        for offset in offsets:
            sends[i, offset] = send(i, source, target, offset, pl.ds(0, rows))
    for offset in one_link + two_links:
        f, n = peers[offset]
        for part, piece in enumerate(pieces[offset]):
            place = (f * near + n, piece)
            loads[offset, part] = own(len(local) + len(loads), keys.at[place], held_keys.at[place])

    def tell(semaphore, devices):
        for device in devices:
            pl.semaphore_signal(
                semaphore, inc=1, device_id=place_of(device), device_id_type=MESH
            )

    def send_straight():
        for root, far_step in ((1 - core, far_index + 1 - core), (core, far_index - core)):
            pltpu.make_async_remote_copy(
                src_ref=keys.at[root * near],
                dst_ref=landed.at[me],
                send_sem=send_sem.at[0, far_step * near + near_index],
                recv_sem=recv_sem.at[0, far_step * near + near_index],
                device_id=place_of((root, 0)),
                device_id_type=MESH,
            ).start()

    barrier = pltpu.get_barrier_semaphore()

    @pl.when(role == SIDE)
    def _():
        @pl.when(odd)
        def _():
            tell(barrier, roots)

        tell(barrier, ends)

        @pl.when(odd)
        def _():
            tell(barrier, [mate])
            pl.semaphore_wait(barrier, len(roots))
            send_straight()

    @pl.when(role == ROOT)
    def _():
        tell(barrier, [mate] + [d for d in sides if d[0] % 2 == 1])

    @pl.when(role == END)
    def _():
        @pl.when(odd)
        def _():
            tell(barrier, [d for d in sides if d[0] % 2 == 0])

        @pl.when(jnp.logical_not(odd))
        def _():
            tell(barrier, [mate])

    straight = {o: jnp.logical_and(role == SIDE, roles[o] == ROOT) for o in one_link}
    for offset, part in sorted(loads, key=lambda at: (at[0] not in first, at[1])):
        load = loads[offset, part].start
        if offset in straight:
            pl.when(jnp.logical_not(straight[offset]))(load)
        else:
            load()
    local[2].start()

    def send_keys(offset):
        for part, place in enumerate(pieces[offset]):
            loads[offset, part].wait()
            send(0, held_keys, landed, offset, place).start()

    def send_to(other, *cores):
        for offset in one_link:
            chosen = roles[offset] == other
            for wanted in cores:
                chosen = jnp.logical_and(chosen, peers[offset][0] % 2 == wanted)
            pl.when(chosen)(functools.partial(send_keys, offset))

    @pl.when(role == SIDE)
    def _():
        @pl.when(odd)
        def _():
            pl.semaphore_wait(link, 1)

        @pl.when(jnp.logical_not(odd))
        def _():
            pl.semaphore_wait(barrier, len(ends) // 2 + 1)

        tell(link, [mate])
        send_to(END, 1)

        @pl.when(jnp.logical_not(odd))
        def _():
            pl.semaphore_wait(link, 1)
            send_straight()

        pl.semaphore_wait(more, len(ends) // 2)
        send_to(END, 0)
        tell(ready, roots + ends)
        pl.semaphore_wait(ready, 1)
        send_to(SIDE)

    @pl.when(role == ROOT)
    def _():
        pl.semaphore_wait(barrier, len(roots) - 1 + len(sides) // 2)
        send_to(SIDE, 1)
        pl.semaphore_wait(ready, len(sides))
        tell(ready, [(d[0] + core, d[1]) for d in sides if d[0] % 2 == 0])
        send_to(SIDE, 0)
        send_to(ROOT)

    @pl.when(role == END)
    def _():
        pl.semaphore_wait(barrier, len(sides) + core)
        pl.when(odd)(functools.partial(tell, more, sides))
        send_to(SIDE)
        pl.semaphore_wait(ready, len(sides))
        send_to(END)

    for offset in two_links:
        send_keys(offset)
    inner = jnp.logical_and(role == SIDE, near_index == 0)
    outward = jnp.logical_and(role != SIDE, jnp.logical_not(odd))
    pairs = [(o, (o[0] + 1, o[1])) for o in one_link if o[0] % 2 == 0]
    across = [pair for pair in pairs if pair[0][0] >= 2]

    def send_values(chosen):
        for low, high in chosen:
            swap = jnp.logical_and(outward, roles[low] == SIDE)
            pl.when(swap)(sends[1, high].start)
            sends[1, low].start()
            pl.when(jnp.logical_not(swap))(sends[1, high].start)

    pl.when(inner)(functools.partial(send_values, across))
    for offset in two_links:
        sends[1, offset].start()
    pl.when(jnp.logical_not(inner))(functools.partial(send_values, across))
    send_values([pair for pair in pairs if pair not in across])
    sends[1, (1, 0)].start()

    for copy in (local[0], local[1], local[3]):
        copy.start()
    for copy in local[:3]:
        copy.wait()

    @pl.loop(0, angles.shape[1] // LANES)
    def _(step):
        start = pl.multiple_of(step * LANES, LANES)
        cosine, sine = cosine_and_sine(angles[:, pl.ds(start, LANES)])
        gain_row = gains[...]
        turn_same = jnp.concatenate([cosine, cosine], axis=0).T * gain_row
        turn_other = jnp.concatenate([-sine, sine], axis=0).T * pltpu.roll(
            gain_row, LANES // 2, 1
        )
        for head in range(heads):
            place = pl.ds(start * heads + head, LANES, stride=heads)
            cosines[place, :] = turn_same
            sines[place, :] = turn_other

    def turn_block(blocks, slot, largest):
        @functools.partial(lax.fori_loop, 0, rows // BLOCK, init_val=largest)
        def result(step, most):
            start = pl.multiple_of(step * BLOCK, BLOCK)
            place = pl.ds(pl.multiple_of(slot * rows + start, BLOCK), BLOCK)
            x = blocks[slot, pl.ds(start, BLOCK), :].astype(jnp.float32)
            mean = jnp.sum(x * x, axis=-1, keepdims=True) * (1.0 / LANES)
            scaled = x * cosines[place, :] + pltpu.roll(x, LANES // 2, 1) * sines[place, :]
            scaled = scaled * lax.rsqrt(mean + 1e-06)
            turned[place, :] = scaled
            return jnp.maximum(
                most, jnp.max(jnp.abs(scaled).reshape(-1, SUBLANES, LANES), axis=0)
            )

        return result

    most = jnp.zeros((SUBLANES, LANES), jnp.float32)
    most = turn_block(held_keys, me, most)
    for offset in sorted(one_link + two_links, key=lambda o: o[0] == 1 and o[1] > 0):
        f, n = peers[offset]
        sends[0, offset].wait_recv()
        most = turn_block(landed, f * near + n, most)
    scale = most[:heads]
    for row in range(heads, SUBLANES, heads):
        scale = jnp.maximum(scale, most[row : row + heads])
    out_scale[...] = scale
    inverse = jnp.concatenate([1.0 / scale] * (SUBLANES // heads), axis=0)[None]

    @pl.loop(0, members * rows // BLOCK)
    def _(step):
        place = pl.ds(pl.multiple_of(step * BLOCK, BLOCK), BLOCK)
        wide = turned[place, :].reshape(-1, SUBLANES, LANES) * inverse
        out_keys[place, :] = wide.reshape(BLOCK, LANES).astype(out_keys.dtype)

    local[3].wait()
    for offset in offsets:
        sends[1, offset].wait_recv()
    for sent in sends.values():
        sent.wait_send()


def hold(x):
    return pltpu.with_memory_space_constraint(x, pltpu.HBM)


def write_out(*refs):
    count = len(refs) // 2
    sources, targets, sems = refs[:count], refs[count : 2 * count], refs[-1]
    copies = [
        pltpu.make_async_copy(source, target, sems.at[i])
        for i, (source, target) in enumerate(zip(sources, targets))
    ]
    for copy in copies:
        copy.start()
    for copy in copies:
        copy.wait()


def shards(far, near, raw_keys, raw_values, turn_angle, key_gain):
    batch, length, heads, size = raw_keys.shape
    members = far * near
    assert batch == members and size == LANES and SUBLANES % heads == 0
    assert far > 2 and near > 1 and far & (far - 1) == 0 and near & (near - 1) == 0
    rows = length * heads
    offsets = [(f, n) for f in range(far) for n in range(near) if (f, n) != (0, 0)]
    offsets.sort(key=lambda o: (o[0] < 2 and o[1] == 0, o[1], o[0]))
    anywhere = pl.BlockSpec(memory_space=pl.ANY)
    inside = pl.BlockSpec(memory_space=pltpu.VMEM)
    results = pl.pallas_call(
        functools.partial(kernel, far, near, heads, offsets),
        out_shape=(
            pltpu.VMEM((members * rows, size), raw_keys.dtype),
            pltpu.VMEM((members, rows, size), raw_values.dtype),
            jax.ShapeDtypeStruct((heads, size), jnp.float32),
        ),
        in_specs=[anywhere] * 4,
        out_specs=(inside, inside, inside),
        scratch_shapes=[
            pltpu.VMEM((members, rows, size), raw_keys.dtype),
            pltpu.VMEM((members, rows, size), raw_keys.dtype),
            pltpu.VMEM((members * rows, size), jnp.float32),
            pltpu.VMEM((members * rows, size), jnp.float32),
            pltpu.VMEM((members * rows, size), jnp.float32),
            pltpu.VMEM((size // 2, members * length), jnp.float32),
            pltpu.VMEM((1, size), jnp.float32),
            pltpu.SemaphoreType.DMA((2, members)),
            pltpu.SemaphoreType.DMA((2, members)),
            pltpu.SemaphoreType.DMA((6 + len(offsets),)),
            pltpu.SemaphoreType.REGULAR,
            pltpu.SemaphoreType.REGULAR,
            pltpu.SemaphoreType.REGULAR,
        ],
        compiler_params=pltpu.CompilerParams(
            collective_id=0, has_side_effects=True, vmem_limit_bytes=32 * 1024 * 1024
        ),
        name="move_and_turn",
    )(
        hold(raw_keys.reshape(batch, rows, size)),
        hold(raw_values.reshape(batch, rows, size)),
        hold(turn_angle.T),
        hold(key_gain.reshape(1, size)),
    )
    narrow_keys, moved_values, key_scale = pl.pallas_call(
        write_out,
        out_shape=tuple(pltpu.HBM(r.shape, r.dtype) for r in results),
        in_specs=[anywhere] * len(results),
        out_specs=(anywhere,) * len(results),
        scratch_shapes=[pltpu.SemaphoreType.DMA((len(results),))],
        compiler_params=pltpu.CompilerParams(vmem_limit_bytes=2 * 1024 * 1024),
        name="write_out",
    )(*results)
    whole = (1, members * length, heads, size)
    return narrow_keys.reshape(whole), moved_values.reshape(whole), key_scale[None]


def solution(mesh):
    in_specs = (
        P(None, ("farcp", "nearcp"), "heads", None),
        P(None, ("farcp", "nearcp"), "heads", None),
        P(),
        P(),
    )
    out_specs = (
        P(("farcp", "nearcp"), None, "heads", None),
        P(("farcp", "nearcp"), None, "heads", None),
        P(("farcp", "nearcp"), "heads", None),
    )
    body = functools.partial(shards, mesh.shape["farcp"], mesh.shape["nearcp"])
    return jax.shard_map(body, mesh=mesh, in_specs=in_specs, out_specs=out_specs, check_vma=False)
```

```python
import functools

import jax
import jax.numpy as jnp
from jax import lax
from jax.experimental import pallas as pl
from jax.experimental.pallas import tpu as pltpu
from jax.sharding import PartitionSpec as P

MESH = pl.DeviceIdType.MESH
LANES = 128
SUBLANES = 8
BLOCK = 128
ROOT, SIDE, END = 0, 1, 2
SINE = (1.0, -0.1666666716337204, 0.008333330973982811, -0.00019840861205011606,
        2.752528644123231e-06, -2.3889498379503493e-08)
COSINE = (1.0, -0.5, 0.0416666679084301, -0.0013888884568586946, 2.4801040126476437e-05,
          -2.752468617472914e-07, 1.9907717696554528e-09)


def polynomial(coefficients, z):
    total = jnp.full_like(z, coefficients[-1])
    for coefficient in coefficients[-2::-1]:
        total = total * z + coefficient
    return total


def cosine_and_sine(angle):
    y = (1.57079637 - jnp.abs(angle)) - 4.371139e-08
    z = y * y
    sine = polynomial(COSINE, z)
    return y * polynomial(SINE, z), jnp.where(angle < 0, -sine, sine)


def partner(index, offset, size):
    result, bit = 0, 1
    while bit < size:
        digit = (index // bit) % 2
        result = result + ((digit + 1) % 2 if offset & bit else digit) * bit
        bit *= 2
    return result


def role_of(far_index, near_index):
    return jnp.where(far_index < 2, 0, 1) + jnp.where(near_index == 0, 0, 1)


def place_of(device):
    return {"farcp": device[0], "nearcp": device[1]}


def kernel(far, near, heads, offsets, keys, values, angle, gain, out_keys, out_values, out_scale,
           landed, held_keys, turned, cosines, sines, angles, gains, send_sem, recv_sem, local_sem,
           ready, link, more):
    members, rows, _ = landed.shape
    far_index, near_index = lax.axis_index("farcp"), lax.axis_index("nearcp")
    me = far_index * near + near_index
    one_link = [o for o in offsets if o[0] < 2 or o[1] == 0]
    two_links = [o for o in offsets if o not in one_link]
    peers = {
        (f, n): (partner(far_index, f, far), partner(near_index, n, near)) for f, n in offsets
    }
    role, roles = role_of(far_index, near_index), {o: role_of(*peers[o]) for o in offsets}
    core = far_index % 2
    odd, mate = core == 1, (far_index + 1 - 2 * core, near_index)
    roots = [(f, 0) for f in range(2)]
    sides = [(f, n) for f in range(2) for n in range(1, near)] + [(f, 0) for f in range(2, far)]
    ends = [(f, n) for f in range(2, far) for n in range(1, near)]

    def own(i, source, target):
        return pltpu.make_async_copy(source, target, local_sem.at[i])

    local = [
        own(0, angle, angles),
        own(1, gain, gains),
        own(2, keys.at[me], held_keys.at[me]),
        own(3, values.at[me], out_values.at[me]),
    ]
    head = rows // 4
    first = ((2, 0), (0, 1))
    pieces = {o: (pl.ds(0, rows),) for o in one_link + two_links}
    for offset in first:
        pieces[offset] = (pl.ds(0, head), pl.ds(head, rows - head))

    def send(i, source, target, offset, place):
        f, n = peers[offset]
        return pltpu.make_async_remote_copy(
            src_ref=source.at[f * near + n, place],
            dst_ref=target.at[me, place],
            send_sem=send_sem.at[i, offset[0] * near + offset[1]],
            recv_sem=recv_sem.at[i, offset[0] * near + offset[1]],
            device_id=place_of((f, n)),
            device_id_type=MESH,
        )

    sends, loads = {}, {}
    for i, (source, target) in enumerate(((held_keys, landed), (values, out_values))):
        for offset in offsets:
            sends[i, offset] = send(i, source, target, offset, pl.ds(0, rows))
    for offset in one_link + two_links:
        f, n = peers[offset]
        for part, piece in enumerate(pieces[offset]):
            place = (f * near + n, piece)
            loads[offset, part] = own(len(local) + len(loads), keys.at[place], held_keys.at[place])

    def tell(semaphore, devices):
        for device in devices:
            pl.semaphore_signal(
                semaphore, inc=1, device_id=place_of(device), device_id_type=MESH
            )

    def send_straight():
        for root, far_step in ((1 - core, far_index + 1 - core), (core, far_index - core)):
            pltpu.make_async_remote_copy(
                src_ref=keys.at[root * near],
                dst_ref=landed.at[me],
                send_sem=send_sem.at[0, far_step * near + near_index],
                recv_sem=recv_sem.at[0, far_step * near + near_index],
                device_id=place_of((root, 0)),
                device_id_type=MESH,
            ).start()

    barrier = pltpu.get_barrier_semaphore()

    @pl.when(role == SIDE)
    def _():
        @pl.when(odd)
        def _():
            tell(barrier, roots)
            pl.semaphore_wait(barrier, len(roots))
            send_straight()
            tell(barrier, [mate])

        tell(barrier, ends)

    @pl.when(role == ROOT)
    def _():
        tell(barrier, [mate] + [d for d in sides if d[0] % 2 == 1])

    straight = {o: jnp.logical_and(role == SIDE, roles[o] == ROOT) for o in one_link}

    def start_loads(chosen):
        for offset, part in chosen:
            load = loads[offset, part].start
            if offset in straight:
                pl.when(jnp.logical_not(straight[offset]))(load)
            else:
                load()

    queue = sorted(loads, key=lambda at: (at[0] not in first, at[1]))
    start_loads(queue[:2])

    @pl.when(role == END)
    def _():
        @pl.when(odd)
        def _():
            tell(barrier, [d for d in sides if d[0] % 2 == 0])

        @pl.when(jnp.logical_not(odd))
        def _():
            tell(barrier, [mate])

    start_loads(queue[2:])
    local[2].start()

    def send_keys(offset):
        for part, place in enumerate(pieces[offset]):
            loads[offset, part].wait()
            send(0, held_keys, landed, offset, place).start()

    def send_to(other, *cores):
        for offset in one_link:
            chosen = roles[offset] == other
            for wanted in cores:
                chosen = jnp.logical_and(chosen, peers[offset][0] % 2 == wanted)
            pl.when(chosen)(functools.partial(send_keys, offset))

    @pl.when(role == SIDE)
    def _():
        @pl.when(odd)
        def _():
            pl.semaphore_wait(link, 1)

        @pl.when(jnp.logical_not(odd))
        def _():
            pl.semaphore_wait(barrier, len(ends) // 2 + 1)

        tell(link, [mate])
        send_to(END, 1)

        @pl.when(jnp.logical_not(odd))
        def _():
            pl.semaphore_wait(link, 1)
            send_straight()

        pl.semaphore_wait(more, len(ends) // 2)
        send_to(END, 0)
        tell(ready, roots + ends)
        pl.semaphore_wait(ready, 1)
        send_to(SIDE)

    @pl.when(role == ROOT)
    def _():
        pl.semaphore_wait(barrier, len(roots) - 1 + len(sides) // 2)
        send_to(SIDE, 1)
        pl.semaphore_wait(ready, len(sides))
        tell(ready, [(d[0] + core, d[1]) for d in sides if d[0] % 2 == 0])
        send_to(SIDE, 0)
        send_to(ROOT)

    @pl.when(role == END)
    def _():
        pl.semaphore_wait(barrier, len(sides) + core)
        pl.when(odd)(functools.partial(tell, more, sides))
        send_to(SIDE)
        pl.semaphore_wait(ready, len(sides))
        send_to(END)

    for offset in two_links:
        send_keys(offset)
    inner = jnp.logical_and(role == SIDE, near_index == 0)
    outward = jnp.logical_and(role != SIDE, jnp.logical_not(odd))
    pairs = [(o, (o[0] + 1, o[1])) for o in one_link if o[0] % 2 == 0]
    across = [pair for pair in pairs if pair[0][0] >= 2]

    def send_values(chosen):
        for low, high in chosen:
            swap = jnp.logical_and(outward, roles[low] == SIDE)
            pl.when(swap)(sends[1, high].start)
            sends[1, low].start()
            pl.when(jnp.logical_not(swap))(sends[1, high].start)

    pl.when(inner)(functools.partial(send_values, across))
    for offset in two_links:
        sends[1, offset].start()
    pl.when(jnp.logical_not(inner))(functools.partial(send_values, across))
    send_values([pair for pair in pairs if pair not in across])
    sends[1, (1, 0)].start()

    for copy in (local[0], local[1], local[3]):
        copy.start()
    for copy in local[:3]:
        copy.wait()

    @pl.loop(0, angles.shape[1] // LANES)
    def _(step):
        start = pl.multiple_of(step * LANES, LANES)
        cosine, sine = cosine_and_sine(angles[:, pl.ds(start, LANES)])
        gain_row = gains[...]
        turn_same = jnp.concatenate([cosine, cosine], axis=0).T * gain_row
        turn_other = jnp.concatenate([-sine, sine], axis=0).T * pltpu.roll(
            gain_row, LANES // 2, 1
        )
        for head in range(heads):
            place = pl.ds(start * heads + head, LANES, stride=heads)
            cosines[place, :] = turn_same
            sines[place, :] = turn_other

    def turn_block(blocks, slot, largest):
        @functools.partial(lax.fori_loop, 0, rows // BLOCK, init_val=largest)
        def result(step, most):
            start = pl.multiple_of(step * BLOCK, BLOCK)
            place = pl.ds(pl.multiple_of(slot * rows + start, BLOCK), BLOCK)
            x = blocks[slot, pl.ds(start, BLOCK), :].astype(jnp.float32)
            mean = jnp.sum(x * x, axis=-1, keepdims=True) * (1.0 / LANES)
            scaled = x * cosines[place, :] + pltpu.roll(x, LANES // 2, 1) * sines[place, :]
            scaled = scaled * lax.rsqrt(mean + 1e-06)
            turned[place, :] = scaled
            return jnp.maximum(
                most, jnp.max(jnp.abs(scaled).reshape(-1, SUBLANES, LANES), axis=0)
            )

        return result

    most = jnp.zeros((SUBLANES, LANES), jnp.float32)
    most = turn_block(held_keys, me, most)
    for offset in sorted(one_link + two_links, key=lambda o: o[0] == 1 and o[1] > 0):
        f, n = peers[offset]
        sends[0, offset].wait_recv()
        most = turn_block(landed, f * near + n, most)
    scale = most[:heads]
    for row in range(heads, SUBLANES, heads):
        scale = jnp.maximum(scale, most[row : row + heads])
    out_scale[...] = scale
    inverse = jnp.concatenate([1.0 / scale] * (SUBLANES // heads), axis=0)[None]

    @pl.loop(0, members * rows // BLOCK)
    def _(step):
        place = pl.ds(pl.multiple_of(step * BLOCK, BLOCK), BLOCK)
        wide = turned[place, :].reshape(-1, SUBLANES, LANES) * inverse
        out_keys[place, :] = wide.reshape(BLOCK, LANES).astype(out_keys.dtype)

    local[3].wait()
    for offset in offsets:
        sends[1, offset].wait_recv()
    for sent in sends.values():
        sent.wait_send()


def hold(x):
    return pltpu.with_memory_space_constraint(x, pltpu.HBM)


def write_out(*refs):
    count = len(refs) // 2
    sources, targets, sems = refs[:count], refs[count : 2 * count], refs[-1]
    copies = [
        pltpu.make_async_copy(source, target, sems.at[i])
        for i, (source, target) in enumerate(zip(sources, targets))
    ]
    for copy in copies:
        copy.start()
    for copy in copies:
        copy.wait()


def shards(far, near, raw_keys, raw_values, turn_angle, key_gain):
    batch, length, heads, size = raw_keys.shape
    members = far * near
    assert batch == members and size == LANES and SUBLANES % heads == 0
    assert far > 2 and near > 1 and far & (far - 1) == 0 and near & (near - 1) == 0
    rows = length * heads
    offsets = [(f, n) for f in range(far) for n in range(near) if (f, n) != (0, 0)]
    offsets.sort(key=lambda o: (o[0] < 2 and o[1] == 0, o[1], o[0]))
    anywhere = pl.BlockSpec(memory_space=pl.ANY)
    inside = pl.BlockSpec(memory_space=pltpu.VMEM)
    results = pl.pallas_call(
        functools.partial(kernel, far, near, heads, offsets),
        out_shape=(
            pltpu.VMEM((members * rows, size), raw_keys.dtype),
            pltpu.VMEM((members, rows, size), raw_values.dtype),
            jax.ShapeDtypeStruct((heads, size), jnp.float32),
        ),
        in_specs=[anywhere] * 4,
        out_specs=(inside, inside, inside),
        scratch_shapes=[
            pltpu.VMEM((members, rows, size), raw_keys.dtype),
            pltpu.VMEM((members, rows, size), raw_keys.dtype),
            pltpu.VMEM((members * rows, size), jnp.float32),
            pltpu.VMEM((members * rows, size), jnp.float32),
            pltpu.VMEM((members * rows, size), jnp.float32),
            pltpu.VMEM((size // 2, members * length), jnp.float32),
            pltpu.VMEM((1, size), jnp.float32),
            pltpu.SemaphoreType.DMA((2, members)),
            pltpu.SemaphoreType.DMA((2, members)),
            pltpu.SemaphoreType.DMA((6 + len(offsets),)),
            pltpu.SemaphoreType.REGULAR,
            pltpu.SemaphoreType.REGULAR,
            pltpu.SemaphoreType.REGULAR,
        ],
        compiler_params=pltpu.CompilerParams(
            collective_id=0, has_side_effects=True, vmem_limit_bytes=32 * 1024 * 1024
        ),
        name="move_and_turn",
    )(
        hold(raw_keys.reshape(batch, rows, size)),
        hold(raw_values.reshape(batch, rows, size)),
        hold(turn_angle.T),
        hold(key_gain.reshape(1, size)),
    )
    narrow_keys, moved_values, key_scale = pl.pallas_call(
        write_out,
        out_shape=tuple(pltpu.HBM(r.shape, r.dtype) for r in results),
        in_specs=[anywhere] * len(results),
        out_specs=(anywhere,) * len(results),
        scratch_shapes=[pltpu.SemaphoreType.DMA((len(results),))],
        compiler_params=pltpu.CompilerParams(vmem_limit_bytes=2 * 1024 * 1024),
        name="write_out",
    )(*results)
    whole = (1, members * length, heads, size)
    return narrow_keys.reshape(whole), moved_values.reshape(whole), key_scale[None]


def solution(mesh):
    in_specs = (
        P(None, ("farcp", "nearcp"), "heads", None),
        P(None, ("farcp", "nearcp"), "heads", None),
        P(),
        P(),
    )
    out_specs = (
        P(("farcp", "nearcp"), None, "heads", None),
        P(("farcp", "nearcp"), None, "heads", None),
        P(("farcp", "nearcp"), "heads", None),
    )
    body = functools.partial(shards, mesh.shape["farcp"], mesh.shape["nearcp"])
    return jax.shard_map(body, mesh=mesh, in_specs=in_specs, out_specs=out_specs, check_vma=False)
```

```python
import functools

import jax
import jax.numpy as jnp
from jax import lax
from jax.experimental import pallas as pl
from jax.experimental.pallas import tpu as pltpu
from jax.sharding import PartitionSpec as P

MESH = pl.DeviceIdType.MESH
LANES = 128
SUBLANES = 8
BLOCK = 128
ROOT, SIDE, END = 0, 1, 2
SINE = (1.0, -0.1666666716337204, 0.008333330973982811, -0.00019840861205011606,
        2.752528644123231e-06, -2.3889498379503493e-08)
COSINE = (1.0, -0.5, 0.0416666679084301, -0.0013888884568586946, 2.4801040126476437e-05,
          -2.752468617472914e-07, 1.9907717696554528e-09)


def polynomial(coefficients, z):
    total = jnp.full_like(z, coefficients[-1])
    for coefficient in coefficients[-2::-1]:
        total = total * z + coefficient
    return total


def cosine_and_sine(angle):
    y = (1.57079637 - jnp.abs(angle)) - 4.371139e-08
    z = y * y
    sine = polynomial(COSINE, z)
    return y * polynomial(SINE, z), jnp.where(angle < 0, -sine, sine)


def partner(index, offset, size):
    result, bit = 0, 1
    while bit < size:
        digit = (index // bit) % 2
        result = result + ((digit + 1) % 2 if offset & bit else digit) * bit
        bit *= 2
    return result


def role_of(far_index, near_index):
    return jnp.where(far_index < 2, 0, 1) + jnp.where(near_index == 0, 0, 1)


def place_of(device):
    return {"farcp": device[0], "nearcp": device[1]}


def kernel(far, near, heads, offsets, keys, values, angle, gain, out_keys, out_values, out_scale,
           landed, held_keys, turned, cosines, sines, angles, gains, send_sem, recv_sem, local_sem,
           ready, link, more):
    members, rows, _ = landed.shape
    far_index, near_index = lax.axis_index("farcp"), lax.axis_index("nearcp")
    me = far_index * near + near_index
    one_link = [o for o in offsets if o[0] < 2 or o[1] == 0]
    two_links = [o for o in offsets if o not in one_link]
    peers = {
        (f, n): (partner(far_index, f, far), partner(near_index, n, near)) for f, n in offsets
    }
    role, roles = role_of(far_index, near_index), {o: role_of(*peers[o]) for o in offsets}
    core = far_index % 2
    odd, mate = core == 1, (far_index + 1 - 2 * core, near_index)
    roots = [(f, 0) for f in range(2)]
    sides = [(f, n) for f in range(2) for n in range(1, near)] + [(f, 0) for f in range(2, far)]
    ends = [(f, n) for f in range(2, far) for n in range(1, near)]

    def own(i, source, target):
        return pltpu.make_async_copy(source, target, local_sem.at[i])

    local = [
        own(0, angle, angles),
        own(1, gain, gains),
        own(2, keys.at[me], held_keys.at[me]),
        own(3, values.at[me], out_values.at[me]),
    ]
    head = rows // 4
    first = ((2, 0), (0, 1))
    pieces = {o: (pl.ds(0, rows),) for o in one_link + two_links}
    for offset in first:
        pieces[offset] = (pl.ds(0, head), pl.ds(head, rows - head))

    def send(i, source, target, offset, place):
        f, n = peers[offset]
        return pltpu.make_async_remote_copy(
            src_ref=source.at[f * near + n, place],
            dst_ref=target.at[me, place],
            send_sem=send_sem.at[i, offset[0] * near + offset[1]],
            recv_sem=recv_sem.at[i, offset[0] * near + offset[1]],
            device_id=place_of((f, n)),
            device_id_type=MESH,
        )

    sends, loads = {}, {}
    for i, (source, target) in enumerate(((held_keys, landed), (values, out_values))):
        for offset in offsets:
            sends[i, offset] = send(i, source, target, offset, pl.ds(0, rows))
    for offset in one_link + two_links:
        f, n = peers[offset]
        for part, piece in enumerate(pieces[offset]):
            place = (f * near + n, piece)
            loads[offset, part] = own(len(local) + len(loads), keys.at[place], held_keys.at[place])

    def tell(semaphore, devices):
        for device in devices:
            pl.semaphore_signal(
                semaphore, inc=1, device_id=place_of(device), device_id_type=MESH
            )

    def send_straight():
        for root, far_step in ((1 - core, far_index + 1 - core), (core, far_index - core)):
            pltpu.make_async_remote_copy(
                src_ref=keys.at[root * near],
                dst_ref=landed.at[me],
                send_sem=send_sem.at[0, far_step * near + near_index],
                recv_sem=recv_sem.at[0, far_step * near + near_index],
                device_id=place_of((root, 0)),
                device_id_type=MESH,
            ).start()

    barrier = pltpu.get_barrier_semaphore()

    @pl.when(role == SIDE)
    def _():
        @pl.when(odd)
        def _():
            tell(barrier, roots)

        tell(barrier, ends)

        @pl.when(odd)
        def _():
            tell(barrier, [mate])
            pl.semaphore_wait(barrier, len(roots))
            send_straight()

    @pl.when(role == ROOT)
    def _():
        tell(barrier, [mate] + [d for d in sides if d[0] % 2 == 1])

    @pl.when(role == END)
    def _():
        @pl.when(odd)
        def _():
            tell(barrier, [d for d in sides if d[0] % 2 == 0])

        @pl.when(jnp.logical_not(odd))
        def _():
            tell(barrier, [mate])

    straight = {o: jnp.logical_and(role == SIDE, roles[o] == ROOT) for o in one_link}
    for offset, part in sorted(loads, key=lambda at: (at[0] not in first, at[1])):
        load = loads[offset, part].start
        if offset in straight:
            pl.when(jnp.logical_not(straight[offset]))(load)
        else:
            load()
    local[2].start()

    def send_keys(offset):
        for part, place in enumerate(pieces[offset]):
            loads[offset, part].wait()
            send(0, held_keys, landed, offset, place).start()

    def send_to(other, *cores):
        for offset in one_link:
            chosen = roles[offset] == other
            for wanted in cores:
                chosen = jnp.logical_and(chosen, peers[offset][0] % 2 == wanted)
            pl.when(chosen)(functools.partial(send_keys, offset))

    @pl.when(role == SIDE)
    def _():
        @pl.when(odd)
        def _():
            pl.semaphore_wait(link, 1)

        @pl.when(jnp.logical_not(odd))
        def _():
            pl.semaphore_wait(barrier, len(ends) // 2 + 1)

        tell(link, [mate])
        send_to(END, 1)

        @pl.when(jnp.logical_not(odd))
        def _():
            pl.semaphore_wait(link, 1)
            send_straight()

        pl.semaphore_wait(more, len(ends) // 2)
        send_to(END, 0)
        tell(ready, roots + ends)
        pl.semaphore_wait(ready, 1)
        send_to(SIDE)

    @pl.when(role == ROOT)
    def _():
        pl.semaphore_wait(barrier, len(roots) - 1 + len(sides) // 2)
        send_to(SIDE, 1)
        pl.semaphore_wait(ready, len(sides))
        tell(ready, [(d[0] + core, d[1]) for d in sides if d[0] % 2 == 0])
        send_to(SIDE, 0)
        send_to(ROOT)

    @pl.when(role == END)
    def _():
        pl.semaphore_wait(barrier, len(sides) + core)
        pl.when(odd)(functools.partial(tell, more, sides))
        send_to(SIDE)
        pl.semaphore_wait(ready, len(sides))
        send_to(END)

    for offset in two_links:
        send_keys(offset)
    inner = jnp.logical_and(role == SIDE, near_index == 0)
    outward = jnp.logical_and(role != SIDE, jnp.logical_not(odd))
    pairs = [(o, (o[0] + 1, o[1])) for o in one_link if o[0] % 2 == 0]
    across = [pair for pair in pairs if pair[0][0] >= 2]

    def send_values(chosen):
        for low, high in chosen:
            beside = jnp.logical_and(roles[low] == SIDE, peers[low][1] == 0)
            swap = jnp.logical_and(outward, beside)
            pl.when(swap)(sends[1, high].start)
            sends[1, low].start()
            pl.when(jnp.logical_not(swap))(sends[1, high].start)

    pl.when(inner)(functools.partial(send_values, across))
    for offset in two_links:
        sends[1, offset].start()
    pl.when(jnp.logical_not(inner))(functools.partial(send_values, across))
    send_values([pair for pair in pairs if pair not in across])
    sends[1, (1, 0)].start()

    for copy in (local[0], local[1], local[3]):
        copy.start()
    for copy in local[:3]:
        copy.wait()

    @pl.loop(0, angles.shape[1] // LANES)
    def _(step):
        start = pl.multiple_of(step * LANES, LANES)
        cosine, sine = cosine_and_sine(angles[:, pl.ds(start, LANES)])
        gain_row = gains[...]
        turn_same = jnp.concatenate([cosine, cosine], axis=0).T * gain_row
        turn_other = jnp.concatenate([-sine, sine], axis=0).T * pltpu.roll(
            gain_row, LANES // 2, 1
        )
        for head in range(heads):
            place = pl.ds(start * heads + head, LANES, stride=heads)
            cosines[place, :] = turn_same
            sines[place, :] = turn_other

    def turn_block(blocks, slot, largest):
        @functools.partial(lax.fori_loop, 0, rows // BLOCK, init_val=largest)
        def result(step, most):
            start = pl.multiple_of(step * BLOCK, BLOCK)
            place = pl.ds(pl.multiple_of(slot * rows + start, BLOCK), BLOCK)
            x = blocks[slot, pl.ds(start, BLOCK), :].astype(jnp.float32)
            mean = jnp.sum(x * x, axis=-1, keepdims=True) * (1.0 / LANES)
            scaled = x * cosines[place, :] + pltpu.roll(x, LANES // 2, 1) * sines[place, :]
            scaled = scaled * lax.rsqrt(mean + 1e-06)
            turned[place, :] = scaled
            return jnp.maximum(
                most, jnp.max(jnp.abs(scaled).reshape(-1, SUBLANES, LANES), axis=0)
            )

        return result

    most = jnp.zeros((SUBLANES, LANES), jnp.float32)
    most = turn_block(held_keys, me, most)
    for offset in sorted(one_link + two_links, key=lambda o: o[0] == 1 and o[1] > 0):
        f, n = peers[offset]
        sends[0, offset].wait_recv()
        most = turn_block(landed, f * near + n, most)
    scale = most[:heads]
    for row in range(heads, SUBLANES, heads):
        scale = jnp.maximum(scale, most[row : row + heads])
    out_scale[...] = scale
    inverse = jnp.concatenate([1.0 / scale] * (SUBLANES // heads), axis=0)[None]

    @pl.loop(0, members * rows // BLOCK)
    def _(step):
        place = pl.ds(pl.multiple_of(step * BLOCK, BLOCK), BLOCK)
        wide = turned[place, :].reshape(-1, SUBLANES, LANES) * inverse
        out_keys[place, :] = wide.reshape(BLOCK, LANES).astype(out_keys.dtype)

    local[3].wait()
    for offset in offsets:
        sends[1, offset].wait_recv()
    for sent in sends.values():
        sent.wait_send()


def hold(x):
    return pltpu.with_memory_space_constraint(x, pltpu.HBM)


def write_out(*refs):
    count = len(refs) // 2
    sources, targets, sems = refs[:count], refs[count : 2 * count], refs[-1]
    copies = [
        pltpu.make_async_copy(source, target, sems.at[i])
        for i, (source, target) in enumerate(zip(sources, targets))
    ]
    for copy in copies:
        copy.start()
    for copy in copies:
        copy.wait()


def shards(far, near, raw_keys, raw_values, turn_angle, key_gain):
    batch, length, heads, size = raw_keys.shape
    members = far * near
    assert batch == members and size == LANES and SUBLANES % heads == 0
    assert far > 2 and near > 1 and far & (far - 1) == 0 and near & (near - 1) == 0
    rows = length * heads
    offsets = [(f, n) for f in range(far) for n in range(near) if (f, n) != (0, 0)]
    offsets.sort(key=lambda o: (o[0] < 2 and o[1] == 0, o[1], o[0]))
    anywhere = pl.BlockSpec(memory_space=pl.ANY)
    inside = pl.BlockSpec(memory_space=pltpu.VMEM)
    results = pl.pallas_call(
        functools.partial(kernel, far, near, heads, offsets),
        out_shape=(
            pltpu.VMEM((members * rows, size), raw_keys.dtype),
            pltpu.VMEM((members, rows, size), raw_values.dtype),
            jax.ShapeDtypeStruct((heads, size), jnp.float32),
        ),
        in_specs=[anywhere] * 4,
        out_specs=(inside, inside, inside),
        scratch_shapes=[
            pltpu.VMEM((members, rows, size), raw_keys.dtype),
            pltpu.VMEM((members, rows, size), raw_keys.dtype),
            pltpu.VMEM((members * rows, size), jnp.float32),
            pltpu.VMEM((members * rows, size), jnp.float32),
            pltpu.VMEM((members * rows, size), jnp.float32),
            pltpu.VMEM((size // 2, members * length), jnp.float32),
            pltpu.VMEM((1, size), jnp.float32),
            pltpu.SemaphoreType.DMA((2, members)),
            pltpu.SemaphoreType.DMA((2, members)),
            pltpu.SemaphoreType.DMA((6 + len(offsets),)),
            pltpu.SemaphoreType.REGULAR,
            pltpu.SemaphoreType.REGULAR,
            pltpu.SemaphoreType.REGULAR,
        ],
        compiler_params=pltpu.CompilerParams(
            collective_id=0, has_side_effects=True, vmem_limit_bytes=32 * 1024 * 1024
        ),
        name="move_and_turn",
    )(
        hold(raw_keys.reshape(batch, rows, size)),
        hold(raw_values.reshape(batch, rows, size)),
        hold(turn_angle.T),
        hold(key_gain.reshape(1, size)),
    )
    narrow_keys, moved_values, key_scale = pl.pallas_call(
        write_out,
        out_shape=tuple(pltpu.HBM(r.shape, r.dtype) for r in results),
        in_specs=[anywhere] * len(results),
        out_specs=(anywhere,) * len(results),
        scratch_shapes=[pltpu.SemaphoreType.DMA((len(results),))],
        compiler_params=pltpu.CompilerParams(vmem_limit_bytes=2 * 1024 * 1024),
        name="write_out",
    )(*results)
    whole = (1, members * length, heads, size)
    return narrow_keys.reshape(whole), moved_values.reshape(whole), key_scale[None]


def solution(mesh):
    in_specs = (
        P(None, ("farcp", "nearcp"), "heads", None),
        P(None, ("farcp", "nearcp"), "heads", None),
        P(),
        P(),
    )
    out_specs = (
        P(("farcp", "nearcp"), None, "heads", None),
        P(("farcp", "nearcp"), None, "heads", None),
        P(("farcp", "nearcp"), "heads", None),
    )
    body = functools.partial(shards, mesh.shape["farcp"], mesh.shape["nearcp"])
    return jax.shard_map(body, mesh=mesh, in_specs=in_specs, out_specs=out_specs, check_vma=False)
```

```python
import functools

import jax
import jax.numpy as jnp
from jax import lax
from jax.experimental import pallas as pl
from jax.experimental.pallas import tpu as pltpu
from jax.sharding import PartitionSpec as P

MESH = pl.DeviceIdType.MESH
LANES = 128
SUBLANES = 8
BLOCK = 128
ROOT, SIDE, END = 0, 1, 2
SINE = (1.0, -0.1666666716337204, 0.008333330973982811, -0.00019840861205011606,
        2.752528644123231e-06, -2.3889498379503493e-08)
COSINE = (1.0, -0.5, 0.0416666679084301, -0.0013888884568586946, 2.4801040126476437e-05,
          -2.752468617472914e-07, 1.9907717696554528e-09)


def polynomial(coefficients, z):
    total = jnp.full_like(z, coefficients[-1])
    for coefficient in coefficients[-2::-1]:
        total = total * z + coefficient
    return total


def cosine_and_sine(angle):
    y = (1.57079637 - jnp.abs(angle)) - 4.371139e-08
    z = y * y
    sine = polynomial(COSINE, z)
    return y * polynomial(SINE, z), jnp.where(angle < 0, -sine, sine)


def partner(index, offset, size):
    result, bit = 0, 1
    while bit < size:
        digit = (index // bit) % 2
        result = result + ((digit + 1) % 2 if offset & bit else digit) * bit
        bit *= 2
    return result


def role_of(far_index, near_index):
    return jnp.where(far_index < 2, 0, 1) + jnp.where(near_index == 0, 0, 1)


def place_of(device):
    return {"farcp": device[0], "nearcp": device[1]}


def kernel(far, near, heads, offsets, keys, values, angle, gain, out_keys, out_values, out_scale,
           landed, held_keys, turned, cosines, sines, angles, gains, send_sem, recv_sem, local_sem,
           ready, link, more):
    members, rows, _ = landed.shape
    far_index, near_index = lax.axis_index("farcp"), lax.axis_index("nearcp")
    me = far_index * near + near_index
    one_link = [o for o in offsets if o[0] < 2 or o[1] == 0]
    two_links = [o for o in offsets if o not in one_link]
    peers = {
        (f, n): (partner(far_index, f, far), partner(near_index, n, near)) for f, n in offsets
    }
    role, roles = role_of(far_index, near_index), {o: role_of(*peers[o]) for o in offsets}
    core = far_index % 2
    odd, mate = core == 1, (far_index + 1 - 2 * core, near_index)
    roots = [(f, 0) for f in range(2)]
    sides = [(f, n) for f in range(2) for n in range(1, near)] + [(f, 0) for f in range(2, far)]
    ends = [(f, n) for f in range(2, far) for n in range(1, near)]

    def own(i, source, target):
        return pltpu.make_async_copy(source, target, local_sem.at[i])

    local = [
        own(0, angle, angles),
        own(1, gain, gains),
        own(2, keys.at[me], held_keys.at[me]),
        own(3, values.at[me], out_values.at[me]),
    ]
    head = rows // 4
    first = ((2, 0), (0, 1))
    pieces = {o: (pl.ds(0, rows),) for o in one_link + two_links}
    for offset in first:
        pieces[offset] = (pl.ds(0, head), pl.ds(head, rows - head))

    def send(i, source, target, offset, place):
        f, n = peers[offset]
        return pltpu.make_async_remote_copy(
            src_ref=source.at[f * near + n, place],
            dst_ref=target.at[me, place],
            send_sem=send_sem.at[i, offset[0] * near + offset[1]],
            recv_sem=recv_sem.at[i, offset[0] * near + offset[1]],
            device_id=place_of((f, n)),
            device_id_type=MESH,
        )

    sends, loads = {}, {}
    for i, (source, target) in enumerate(((held_keys, landed), (values, out_values))):
        for offset in offsets:
            sends[i, offset] = send(i, source, target, offset, pl.ds(0, rows))
    for offset in one_link + two_links:
        f, n = peers[offset]
        for part, piece in enumerate(pieces[offset]):
            place = (f * near + n, piece)
            loads[offset, part] = own(len(local) + len(loads), keys.at[place], held_keys.at[place])

    def tell(semaphore, devices):
        for device in devices:
            pl.semaphore_signal(
                semaphore, inc=1, device_id=place_of(device), device_id_type=MESH
            )

    def send_straight():
        for root, far_step in ((1 - core, far_index + 1 - core), (core, far_index - core)):
            pltpu.make_async_remote_copy(
                src_ref=keys.at[root * near],
                dst_ref=landed.at[me],
                send_sem=send_sem.at[0, far_step * near + near_index],
                recv_sem=recv_sem.at[0, far_step * near + near_index],
                device_id=place_of((root, 0)),
                device_id_type=MESH,
            ).start()

    barrier = pltpu.get_barrier_semaphore()

    @pl.when(role == SIDE)
    def _():
        @pl.when(odd)
        def _():
            tell(barrier, roots)

        tell(barrier, ends)

        @pl.when(odd)
        def _():
            tell(barrier, [mate])
            pl.semaphore_wait(barrier, len(roots))
            send_straight()

    @pl.when(role == ROOT)
    def _():
        tell(barrier, [mate] + [d for d in sides if d[0] % 2 == 1])

    @pl.when(role == END)
    def _():
        @pl.when(odd)
        def _():
            tell(barrier, [d for d in sides if d[0] % 2 == 0])

        @pl.when(jnp.logical_not(odd))
        def _():
            tell(barrier, [mate])

    straight = {o: jnp.logical_and(role == SIDE, roles[o] == ROOT) for o in one_link}
    for offset, part in sorted(loads, key=lambda at: (at[0] not in first, at[1])):
        load = loads[offset, part].start
        if offset in straight:
            pl.when(jnp.logical_not(straight[offset]))(load)
        else:
            load()
    local[2].start()

    def send_keys(offset):
        for part, place in enumerate(pieces[offset]):
            loads[offset, part].wait()
            send(0, held_keys, landed, offset, place).start()

    def send_to(other, *cores):
        for offset in one_link:
            chosen = roles[offset] == other
            for wanted in cores:
                chosen = jnp.logical_and(chosen, peers[offset][0] % 2 == wanted)
            pl.when(chosen)(functools.partial(send_keys, offset))

    @pl.when(role == SIDE)
    def _():
        @pl.when(odd)
        def _():
            pl.semaphore_wait(link, 1)

        @pl.when(jnp.logical_not(odd))
        def _():
            pl.semaphore_wait(barrier, len(ends) // 2 + 1)

        tell(link, [mate])
        send_to(END, 1)

        @pl.when(jnp.logical_not(odd))
        def _():
            pl.semaphore_wait(link, 1)
            send_straight()

        pl.semaphore_wait(more, len(ends) // 2)
        send_to(END, 0)
        tell(ready, roots + ends)
        pl.semaphore_wait(ready, 1)
        send_to(SIDE)

    @pl.when(role == ROOT)
    def _():
        pl.semaphore_wait(barrier, len(roots) - 1 + len(sides) // 2)
        send_to(SIDE, 1)
        pl.semaphore_wait(ready, len(sides))
        tell(ready, [(d[0] + core, d[1]) for d in sides if d[0] % 2 == 0])
        send_to(SIDE, 0)
        send_to(ROOT)

    @pl.when(role == END)
    def _():
        pl.semaphore_wait(barrier, len(sides) + core)
        pl.when(odd)(functools.partial(tell, more, sides))
        send_to(SIDE)
        pl.semaphore_wait(ready, len(sides))
        send_to(END)

    for offset in two_links:
        send_keys(offset)
    inner = jnp.logical_and(role == SIDE, near_index == 0)
    outward = jnp.logical_and(role != SIDE, jnp.logical_not(odd))
    pairs = [(o, (o[0] + 1, o[1])) for o in one_link if o[0] % 2 == 0]
    across = [pair for pair in pairs if pair[0][0] >= 2]

    def send_values(chosen):
        for low, high in chosen:
            beside = jnp.logical_and(roles[low] == SIDE, peers[low][1] == 0)
            swap = jnp.logical_and(outward, beside)
            pl.when(swap)(sends[1, high].start)
            sends[1, low].start()
            pl.when(jnp.logical_not(swap))(sends[1, high].start)

    pl.when(inner)(functools.partial(send_values, across))
    for offset in two_links:
        sends[1, offset].start()
    send_values([pair for pair in pairs if pair not in across])
    pl.when(jnp.logical_not(inner))(functools.partial(send_values, across))
    sends[1, (1, 0)].start()

    for copy in (local[0], local[1], local[3]):
        copy.start()
    for copy in local[:3]:
        copy.wait()

    @pl.loop(0, angles.shape[1] // LANES)
    def _(step):
        start = pl.multiple_of(step * LANES, LANES)
        cosine, sine = cosine_and_sine(angles[:, pl.ds(start, LANES)])
        gain_row = gains[...]
        turn_same = jnp.concatenate([cosine, cosine], axis=0).T * gain_row
        turn_other = jnp.concatenate([-sine, sine], axis=0).T * pltpu.roll(
            gain_row, LANES // 2, 1
        )
        for head in range(heads):
            place = pl.ds(start * heads + head, LANES, stride=heads)
            cosines[place, :] = turn_same
            sines[place, :] = turn_other

    def turn_block(blocks, slot, largest):
        @functools.partial(lax.fori_loop, 0, rows // BLOCK, init_val=largest)
        def result(step, most):
            start = pl.multiple_of(step * BLOCK, BLOCK)
            place = pl.ds(pl.multiple_of(slot * rows + start, BLOCK), BLOCK)
            x = blocks[slot, pl.ds(start, BLOCK), :].astype(jnp.float32)
            mean = jnp.sum(x * x, axis=-1, keepdims=True) * (1.0 / LANES)
            scaled = x * cosines[place, :] + pltpu.roll(x, LANES // 2, 1) * sines[place, :]
            scaled = scaled * lax.rsqrt(mean + 1e-06)
            turned[place, :] = scaled
            return jnp.maximum(
                most, jnp.max(jnp.abs(scaled).reshape(-1, SUBLANES, LANES), axis=0)
            )

        return result

    most = jnp.zeros((SUBLANES, LANES), jnp.float32)
    most = turn_block(held_keys, me, most)
    for offset in sorted(one_link + two_links, key=lambda o: o[0] == 1 and o[1] > 0):
        f, n = peers[offset]
        sends[0, offset].wait_recv()
        most = turn_block(landed, f * near + n, most)
    scale = most[:heads]
    for row in range(heads, SUBLANES, heads):
        scale = jnp.maximum(scale, most[row : row + heads])
    out_scale[...] = scale
    inverse = jnp.concatenate([1.0 / scale] * (SUBLANES // heads), axis=0)[None]

    @pl.loop(0, members * rows // BLOCK)
    def _(step):
        place = pl.ds(pl.multiple_of(step * BLOCK, BLOCK), BLOCK)
        wide = turned[place, :].reshape(-1, SUBLANES, LANES) * inverse
        out_keys[place, :] = wide.reshape(BLOCK, LANES).astype(out_keys.dtype)

    local[3].wait()
    for offset in offsets:
        sends[1, offset].wait_recv()
    for sent in sends.values():
        sent.wait_send()


def hold(x):
    return pltpu.with_memory_space_constraint(x, pltpu.HBM)


def write_out(*refs):
    count = len(refs) // 2
    sources, targets, sems = refs[:count], refs[count : 2 * count], refs[-1]
    copies = [
        pltpu.make_async_copy(source, target, sems.at[i])
        for i, (source, target) in enumerate(zip(sources, targets))
    ]
    for copy in copies:
        copy.start()
    for copy in copies:
        copy.wait()


def shards(far, near, raw_keys, raw_values, turn_angle, key_gain):
    batch, length, heads, size = raw_keys.shape
    members = far * near
    assert batch == members and size == LANES and SUBLANES % heads == 0
    assert far > 2 and near > 1 and far & (far - 1) == 0 and near & (near - 1) == 0
    rows = length * heads
    offsets = [(f, n) for f in range(far) for n in range(near) if (f, n) != (0, 0)]
    offsets.sort(key=lambda o: (o[0] < 2 and o[1] == 0, o[1], o[0]))
    anywhere = pl.BlockSpec(memory_space=pl.ANY)
    inside = pl.BlockSpec(memory_space=pltpu.VMEM)
    results = pl.pallas_call(
        functools.partial(kernel, far, near, heads, offsets),
        out_shape=(
            pltpu.VMEM((members * rows, size), raw_keys.dtype),
            pltpu.VMEM((members, rows, size), raw_values.dtype),
            jax.ShapeDtypeStruct((heads, size), jnp.float32),
        ),
        in_specs=[anywhere] * 4,
        out_specs=(inside, inside, inside),
        scratch_shapes=[
            pltpu.VMEM((members, rows, size), raw_keys.dtype),
            pltpu.VMEM((members, rows, size), raw_keys.dtype),
            pltpu.VMEM((members * rows, size), jnp.float32),
            pltpu.VMEM((members * rows, size), jnp.float32),
            pltpu.VMEM((members * rows, size), jnp.float32),
            pltpu.VMEM((size // 2, members * length), jnp.float32),
            pltpu.VMEM((1, size), jnp.float32),
            pltpu.SemaphoreType.DMA((2, members)),
            pltpu.SemaphoreType.DMA((2, members)),
            pltpu.SemaphoreType.DMA((6 + len(offsets),)),
            pltpu.SemaphoreType.REGULAR,
            pltpu.SemaphoreType.REGULAR,
            pltpu.SemaphoreType.REGULAR,
        ],
        compiler_params=pltpu.CompilerParams(
            collective_id=0, has_side_effects=True, vmem_limit_bytes=32 * 1024 * 1024
        ),
        name="move_and_turn",
    )(
        hold(raw_keys.reshape(batch, rows, size)),
        hold(raw_values.reshape(batch, rows, size)),
        hold(turn_angle.T),
        hold(key_gain.reshape(1, size)),
    )
    narrow_keys, moved_values, key_scale = pl.pallas_call(
        write_out,
        out_shape=tuple(pltpu.HBM(r.shape, r.dtype) for r in results),
        in_specs=[anywhere] * len(results),
        out_specs=(anywhere,) * len(results),
        scratch_shapes=[pltpu.SemaphoreType.DMA((len(results),))],
        compiler_params=pltpu.CompilerParams(vmem_limit_bytes=2 * 1024 * 1024),
        name="write_out",
    )(*results)
    whole = (1, members * length, heads, size)
    return narrow_keys.reshape(whole), moved_values.reshape(whole), key_scale[None]


def solution(mesh):
    in_specs = (
        P(None, ("farcp", "nearcp"), "heads", None),
        P(None, ("farcp", "nearcp"), "heads", None),
        P(),
        P(),
    )
    out_specs = (
        P(("farcp", "nearcp"), None, "heads", None),
        P(("farcp", "nearcp"), None, "heads", None),
        P(("farcp", "nearcp"), "heads", None),
    )
    body = functools.partial(shards, mesh.shape["farcp"], mesh.shape["nearcp"])
    return jax.shard_map(body, mesh=mesh, in_specs=in_specs, out_specs=out_specs, check_vma=False)
```
